32 devices in a mesh: row: 4 (over z), col: 2 (over y), dp: 4 (over x, core).
Axes of the slice: x: 2, y: 2, z: 4, core: 2. Of those that a mesh axis runs over, the one named last changes fastest.
Arguments:
- inputs: bfloat16 [4096, 4096], P('dp', 'row'), may hold values from -6 to 6
- upstream: bfloat16 [4096, 4096], P('dp', 'row'), may hold values from -6 to 6
- expand: bfloat16 [4096, 16384], P('row', 'col'), may hold values from -0.09375 to 0.09375
- biases: float32 [16384], P('col'), may hold values from -5 to 5
- contract: bfloat16 [16384, 4096], P('col', 'row'), may hold values from -0.046875 to 0.046875
Outputs:
- grad_inputs: bfloat16 [4096, 4096], P('dp', 'row')
- grad_expand: bfloat16 [4096, 16384], P('row', 'col')
- grad_biases: bfloat16 [16384], P('col')
- grad_contract: bfloat16 [16384, 4096], P('col', 'row')
- grad_offset: bfloat16 [4096], P('row')
The draws below stay inside these ranges and needn't reach their ends.
All inputs are finite; a program needn't handle non-finite values.
Results may differ from the reference program's by a relative error of at most 0.022.
Values may be sent and summed in bfloat16 or wider, within the bound.
A program may use at most 192 MiB of HBM per device.

```python
import jax
import jax.numpy as jnp
from jax import lax

D = 4096
FF = 16384
TOK_DEV = 1024
TOKENS = 4096
N_ROW = 4
N_COL = 2
N_DP = 4


def levels(rng, extent, pieces, least, largest):
    level = 1.0
    for dim, parts in pieces:
        heights = jax.random.uniform(jax.random.fold_in(jax.random.fold_in(rng, 6), dim), (parts,), jnp.float32, least / len(pieces), largest / len(pieces))
        level = level * jnp.repeat(jnp.exp(heights), extent[dim] // parts).reshape((-1,) + (1,) * (len(extent) - 1 - dim))
    return level


def centred(own_key, dims, deviation, most, shards=(), kind=jnp.bfloat16):
    loudness = levels(own_key, dims, shards, -0.22, 0.18) if shards else 1.0
    entries = jax.random.normal(own_key, dims, jnp.float32) * deviation * loudness
    return jnp.minimum(jnp.maximum(entries, -most), most).astype(kind)


def setup_inputs(seed: int = 0) -> dict:
    splits = jax.random.split(jax.random.key(seed), 6)
    return {
        "inputs": centred(splits[0], (TOKENS, D), 1.0, 6.0, ((0, 4), (1, 4))),
        "upstream": centred(splits[1], (TOKENS, D), 1.0, 6.0, ((0, 4), (1, 4))),
        "expand": centred(splits[2], (D, FF), D ** -0.5, 0.09375, ((0, 4), (1, 2))),
        "biases": centred(splits[3], (FF,), 1.0, 5.0, ((0, 2),), jnp.float32),
        "contract": centred(splits[4], (FF, D), FF ** -0.5, 0.046875, ((0, 2), (1, 4))),
    }


def gelu_tanh(values):
    return jax.nn.gelu(values, approximate=True)

def rounded(values):
    return lax.optimization_barrier(values.astype(jnp.bfloat16)).astype(jnp.float32)

def reference(inputs, upstream, expand, biases, contract):
    width = D // N_ROW
    hidden_width = FF // N_COL
    pre_sum = jnp.zeros((TOKENS, FF), jnp.float32)
    back_sum = jnp.zeros((TOKENS, FF), jnp.float32)
    for index in range(N_ROW):
        first = index * width
        pre_part = jnp.dot(inputs[:, first:first + width], expand[first:first + width, :], preferred_element_type=jnp.float32)
        pre_sum = pre_sum + rounded(pre_part)
        back_part = jnp.dot(upstream[:, first:first + width], contract[:, first:first + width].T, preferred_element_type=jnp.float32)
        back_sum = back_sum + rounded(back_part)
    hidden = (pre_sum + biases[None, :]).astype(jnp.bfloat16)
    backward = back_sum.astype(jnp.bfloat16)
    forward_act, pullback = jax.vjp(gelu_tanh, hidden.astype(jnp.float32))
    slope_grad, = pullback(backward.astype(jnp.float32))
    activation = forward_act.astype(jnp.bfloat16)
    hidden_grad = slope_grad.astype(jnp.bfloat16)
    input_total = jnp.zeros((TOKENS, D), jnp.float32)
    for index in range(N_COL):
        first = index * hidden_width
        input_part = jnp.dot(hidden_grad[:, first:first + hidden_width], expand[:, first:first + hidden_width].T, preferred_element_type=jnp.float32)
        input_total = input_total + rounded(input_part)
    grad_inputs = input_total.astype(jnp.bfloat16)
    factor = TOKENS ** (-0.5)
    expand_total = jnp.zeros((D, FF), jnp.float32)
    biases_total = jnp.zeros((FF,), jnp.float32)
    contract_total = jnp.zeros((FF, D), jnp.float32)
    offset_total = jnp.zeros((D,), jnp.float32)
    for index in range(N_DP):
        first = index * TOK_DEV
        input_block = inputs[first:first + TOK_DEV]
        grad_block = hidden_grad[first:first + TOK_DEV]
        active_block = activation[first:first + TOK_DEV]
        upstream_block = upstream[first:first + TOK_DEV]
        expand_total = expand_total + rounded(jnp.dot(input_block.T, grad_block, preferred_element_type=jnp.float32) * factor)
        biases_total = biases_total + rounded(lax.optimization_barrier(jnp.sum(grad_block, axis=0, dtype=jnp.float32)) * factor)
        contract_total = contract_total + rounded(jnp.dot(active_block.T, upstream_block, preferred_element_type=jnp.float32) * factor)
        offset_total = offset_total + rounded(lax.optimization_barrier(jnp.sum(upstream_block, axis=0, dtype=jnp.float32)) * factor)
    return (grad_inputs, expand_total.astype(jnp.bfloat16), biases_total.astype(jnp.bfloat16), contract_total.astype(jnp.bfloat16), offset_total.astype(jnp.bfloat16))
```

```python
import functools

import jax
import jax.numpy as jnp
from jax import lax
from jax.experimental import pallas as pl
from jax.experimental.pallas import tpu as pltpu
from jax.sharding import PartitionSpec as P

LANES = 128
F32 = jnp.float32
BF16 = jnp.bfloat16


def gelu_tanh(values):
    return jax.nn.gelu(values, approximate=True)


def pointwise(hidden, backward):
    forward_act, pullback = jax.vjp(gelu_tanh, hidden.astype(F32))
    (slope_grad,) = pullback(backward.astype(F32))
    return (forward_act.astype(BF16), slope_grad.astype(BF16))


def swap(value, axis, distance):
    n = lax.axis_size(axis)
    return lax.ppermute(value, axis, [(i, i ^ distance) for i in range(n)])


def bits(axis):
    n = lax.axis_size(axis)
    assert n & (n - 1) == 0
    return [1 << b for b in range(n.bit_length() - 1)]


def dp_order():
    order = [0]
    for b in reversed(bits("dp")):
        order = order + [j ^ b for j in order]
    return order


def dot(a, b, ca, cb):
    return lax.dot_general(a, b, (((ca,), (cb,)), ((), ())), preferred_element_type=F32)


def pick(array, index, axis, width, sends):
    other = array.shape[1 - axis]
    total = index.shape[0]
    joined = total - sends
    if width % LANES:
        parts = [
            lax.dynamic_slice_in_dim(array, index[t] * width, width, axis=axis) for t in range(total)
        ]
        return parts[:sends] + [jnp.concatenate(parts[sends:], axis=axis)]
    steps = 4 if other % (4 * LANES) == 0 else 1
    size = other // steps

    def kernel(index_ref, *refs):
        ins, outs = refs[:total], refs[total:]
        for t in range(total):
            if t < sends:
                outs[t][...] = ins[t][...]
            else:
                at = pl.ds((t - sends) * width, width)
                if axis == 1:
                    outs[sends][:, at] = ins[t][...]
                else:
                    outs[sends][at, :] = ins[t][...]

    def spec(t):
        if axis == 1:
            return pl.BlockSpec((size, width), lambda g, idx: (g, idx[t]))
        return pl.BlockSpec((width, size), lambda g, idx: (idx[t], g))

    def out_spec(count):
        if axis == 1:
            return pl.BlockSpec((size, count * width), lambda g, idx: (g, 0))
        return pl.BlockSpec((count * width, size), lambda g, idx: (0, g))

    def out_type(count):
        shape = (other, count * width) if axis == 1 else (count * width, other)
        return jax.ShapeDtypeStruct(shape, array.dtype)

    counts = [1] * sends + [joined]
    moved = 2 * total * width * other * array.dtype.itemsize
    return pl.pallas_call(
        kernel,
        grid_spec=pltpu.PrefetchScalarGridSpec(
            num_scalar_prefetch=1,
            grid=(steps,),
            in_specs=[spec(t) for t in range(total)],
            out_specs=[out_spec(c) for c in counts],
        ),
        out_shape=[out_type(c) for c in counts],
        cost_estimate=pl.CostEstimate(flops=moved, bytes_accessed=moved, transcendentals=0),
        name="pick",
    )(index, *([array] * total))


def place(target, kept, got, index, axis, shape):
    half, n, rows, cols = kept.shape
    width = cols if axis == 1 else rows
    i = lax.axis_index("dp")
    odd = (i % 2).astype(jnp.int32)
    if axis == 1 and (2 * width) % LANES:
        target = jnp.zeros(shape, kept.dtype) if target is None else target
        first = jnp.where(odd == 0, kept, got)
        second = jnp.where(odd == 0, got, kept)
        for d in range(n):
            for p in range(half):
                pair = jnp.concatenate([first[p, d], second[p, d]], axis=axis)
                target = lax.dynamic_update_slice_in_dim(
                    target, pair, index[d * half + p] * 2 * width, axis=axis
                )
        return target

    def kernel(index_ref, *refs):
        a, b, out = refs[0], refs[1], refs[-1]
        is_odd = index_ref[n * half] == 1

        def put(lo, hi):
            if axis == 1:
                out[:, :width] = lo[0, 0]
                out[:, width:] = hi[0, 0]
            else:
                out[:width, :] = lo[0, 0]
                out[width:, :] = hi[0, 0]

        @pl.when(is_odd)
        def _():
            put(b, a)

        @pl.when(jnp.logical_not(is_odd))
        def _():
            put(a, b)

    spec = pl.BlockSpec((1, 1, rows, cols), lambda d, p, idx: (p, d, 0, 0))
    if axis == 1:
        out_spec = pl.BlockSpec((rows, 2 * width), lambda d, p, idx: (0, idx[d * half + p]))
    else:
        out_spec = pl.BlockSpec((2 * width, cols), lambda d, p, idx: (idx[d * half + p], 0))
    extra = [] if target is None else [target]
    moved = 2 * kept.size * 2 * kept.dtype.itemsize
    return pl.pallas_call(
        kernel,
        grid_spec=pltpu.PrefetchScalarGridSpec(
            num_scalar_prefetch=1,
            grid=(n, half),
            in_specs=[spec, spec] + [pl.BlockSpec(memory_space=pl.ANY)] * len(extra),
            out_specs=out_spec,
        ),
        out_shape=jax.ShapeDtypeStruct(shape, kept.dtype),
        input_output_aliases={3: 0} if extra else {},
        cost_estimate=pl.CostEstimate(flops=moved, bytes_accessed=moved, transcendentals=0),
        name="place",
    )(jnp.concatenate([index, odd[None]]), kept, got, *extra)


def gather_tokens(array):
    n, k = lax.axis_size("row"), lax.axis_size("col")
    y = lax.axis_index("col")
    piece = array.shape[0] // k
    pieces = [lax.dynamic_slice_in_dim(array, (y ^ e) * piece, piece, axis=0) for e in range(k)]
    rows = [[p] for p in pieces]
    for d in range(1, n):
        own = swap(pieces[0], "row", d)
        rows[0].append(own)
        for e in range(1, k):
            rows[e].append(swap(own, "col", e))
    return jnp.concatenate([jnp.concatenate(r, axis=1) for r in rows], axis=0)


def join_dp(part, axis):
    for b in reversed(bits("dp")):
        part = jnp.concatenate([part, swap(part, "dp", b)], axis=axis)
    return part


def reduce_dp(part, axis):
    for b in bits("dp"):
        half = part.shape[axis] // 2
        keep = lax.slice_in_dim(part, 0, half, axis=axis)
        got = swap(lax.slice_in_dim(part, half, 2 * half, axis=axis), "dp", b)
        part = (keep.astype(F32) + got.astype(F32)).astype(BF16)
    return part


def spread(part, axis):
    n = lax.axis_size("row")
    block = part.shape[1 - axis] // n
    cut = [lax.slice_in_dim(part, d * block, (d + 1) * block, axis=1 - axis) for d in range(n)]
    mine = jnp.stack([cut[0]] + [swap(cut[d], "row", d) for d in range(1, n)])[None]
    order = list(reversed(bits("dp")))
    for b in order[:-1]:
        mine = jnp.concatenate([mine, swap(mine, "dp", b)], axis=0)
    return mine, swap(mine, "dp", order[-1])


def local(inputs, upstream, expand, biases, contract):
    n, k, q = lax.axis_size("row"), lax.axis_size("col"), lax.axis_size("dp")
    z, y, i = lax.axis_index("row"), lax.axis_index("col"), lax.axis_index("dp")
    tokens, block = inputs.shape
    width = expand.shape[1]
    factor = (tokens * q) ** (-0.5)
    own_width = width // n
    chunks = max(1, own_width // (q * LANES))
    chunk = own_width // chunks
    quarter = chunk // q
    order = dp_order()

    inputs_all = gather_tokens(inputs)
    upstream_all = gather_tokens(upstream)

    def source(c):
        far = [((z ^ d) * chunks + c) * q + i for d in range(1, n)]
        near = [(z * chunks + c) * q + (i ^ j) for j in order]
        return jnp.stack(far + near).astype(jnp.int32)

    def goal(c):
        half = order[: q // 2]
        return jnp.stack(
            [(((z ^ d) * chunks + c) * q + (i ^ j)) // 2 for d in range(n) for j in half]
        ).astype(jnp.int32)

    bias_rows = []
    grad_expand = grad_contract = share = None
    for c in range(chunks):
        index = source(c)
        *far_e, near_e = pick(expand, index, 1, quarter, n - 1)
        *far_c, near_c = pick(contract, index, 0, quarter, n - 1)
        rest_e = jnp.concatenate([swap(far_e[d - 1], "row", d) for d in range(1, n)], axis=0)
        rest_c = jnp.concatenate([swap(far_c[d - 1], "row", d) for d in range(1, n)], axis=1)
        expand_c = jnp.concatenate([near_e, join_dp(rest_e, 1)], axis=0)
        contract_c = jnp.concatenate([near_c, join_dp(rest_c, 0)], axis=1)
        near = [lax.dynamic_slice_in_dim(biases, index[n - 1 + t] * quarter, quarter) for t in range(q)]
        pre = dot(inputs_all, expand_c, 1, 0)
        back = dot(upstream_all, contract_c, 1, 1).astype(BF16)
        hidden = (pre + jnp.concatenate(near)[None, :]).astype(BF16)
        active, grad = pointwise(hidden, back)
        contract_part = (dot(active, upstream_all, 0, 0) * factor).astype(BF16)
        expand_part = (dot(inputs_all, grad, 0, 0) * factor).astype(BF16)
        bias_rows.append((jnp.sum(grad, axis=0, dtype=F32) * factor).astype(BF16).astype(F32))
        kept, got = spread(reduce_dp(contract_part, 0), 0)
        grad_contract = place(grad_contract, kept, got, goal(c), 0, contract.shape)
        kept, got = spread(reduce_dp(expand_part, 1), 1)
        grad_expand = place(grad_expand, kept, got, goal(c), 1, expand.shape)
        term = dot(grad, expand_c, 1, 1)
        share = term if share is None else share + term

    piece = tokens // k
    share = share.astype(BF16)
    total = share[:piece].astype(F32)
    for e in range(1, k):
        total = total + swap(share[e * piece : (e + 1) * piece], "col", e).astype(F32)
    total = total.astype(BF16)
    mine = total[:, :block].astype(F32)
    for d in range(1, n):
        mine = mine + swap(total[:, d * block : (d + 1) * block], "row", d).astype(F32)
    mine = mine.astype(BF16)
    grad_inputs = jnp.zeros((tokens, block), BF16)
    for e in range(k):
        got = mine if e == 0 else swap(mine, "col", e)
        grad_inputs = lax.dynamic_update_slice_in_dim(grad_inputs, got, (y ^ e) * piece, axis=0)

    vector = jnp.zeros((width + n * block,), F32)
    for c in range(chunks):
        for t, j in enumerate(order):
            at = (((z * chunks + c) * q) + (i ^ j)) * quarter
            vector = lax.dynamic_update_slice_in_dim(
                vector, bias_rows[c][t * quarter : (t + 1) * quarter], at, axis=0
            )
    offset = (jnp.sum(upstream, axis=0, dtype=F32) * factor).astype(BF16).astype(F32)
    vector = lax.dynamic_update_slice_in_dim(vector, offset, width + z * block, axis=0)
    vector = lax.psum(vector, ("row", "dp"))
    grad_biases = vector[:width].astype(BF16)
    grad_offset = lax.dynamic_slice_in_dim(vector, width + z * block, block, axis=0).astype(BF16)
    return (grad_inputs, grad_expand, grad_biases, grad_contract, grad_offset)


def fused_local(inputs, upstream, expand, biases, contract):
    n, k, q = lax.axis_size("row"), lax.axis_size("col"), lax.axis_size("dp")
    tokens, block = inputs.shape
    model = n * block
    width = expand.shape[1]
    own_width = width // n
    quarter = LANES
    chunk = q * quarter
    chunks = own_width // chunk
    half = tokens // k
    factor = (tokens * q) ** (-0.5)
    c0 = 0.7978845608028654
    c1 = 0.044715
    token_tile = 256 if tokens % 256 == 0 else tokens
    model_tile = 512 if block % 512 == 0 else block

    def kernel(
        x_ref, u_ref, e_ref, bias_ref, t_ref,
        gx_ref, ge_ref, gt_ref, gb_ref,
        we_ref, wt_ref, r1e_ref, r1t_ref, r2e_ref, r2t_ref, s1_ref, s2_ref,
        x_all, u_all, e_buf, t_buf, act, act_t, hg, pe, pt, tmp_e, tmp_t, gx_all,
        line_s, line_r, y_s, y_r, send, recv, gi_s, gi_r, loc,
    ):
        z, y, i = lax.axis_index("row"), lax.axis_index("col"), lax.axis_index("dp")
        core, far = lax.rem(i, 2), lax.div(i, 2)
        r = core * 2 + far
        core_to = {"dp": far * 2 + (1 - core)}
        far_to = {"dp": (1 - far) * 2 + core}
        y_to = {"col": 1 - y}

        def row(d):
            return lax.rem(z + d, n)

        def span(start, size):
            return pl.ds(pl.multiple_of(start, size), size)

        def push(src, dst, ss, rs, to):
            pltpu.make_async_remote_copy(
                src_ref=src, dst_ref=dst, send_sem=ss, recv_sem=rs,
                device_id=to, device_id_type=pl.DeviceIdType.MESH,
            ).start()

        def wait(region, sem):
            pltpu.make_async_copy(region, region, sem).wait()

        barrier = pltpu.get_barrier_semaphore()
        partners = [{"row": row(d)} for d in range(1, n)] + [y_to, core_to, far_to]
        for to in partners:
            pl.semaphore_signal(barrier, inc=1, device_id=to, device_id_type=pl.DeviceIdType.MESH)
        pl.semaphore_wait(barrier, len(partners))

        arrays = ((x_ref, x_all), (u_ref, u_all))
        mine = span(y * half, half)
        own_loads = [
            pltpu.make_async_copy(a, full.at[:, span(z * block, block)], loc.at[m])
            for m, (a, full) in enumerate(arrays)
        ]
        for copy in own_loads:
            copy.start()

        wz, wx, wc, wf, rc, rx, az, ax, ac, af = range(10)

        def weight_at(m, c, b, s):
            if m == 0:
                return we_ref.at[c, span(b * block, block), span(s * quarter, quarter)]
            return wt_ref.at[c, span(s * quarter, quarter), span(b * block, block)]

        def weight_from(m, b, c, s):
            at = span(((b * chunks + c) * q + s) * quarter, quarter)
            return e_ref.at[:, at] if m == 0 else t_ref.at[at, :]

        def weight_bytes(m, c):
            if m == 0:
                return we_ref.at[c, pl.ds(0, (n - 1) * block), pl.ds(0, quarter)]
            return wt_ref.at[c, pl.ds(0, quarter), pl.ds(0, (n - 1) * block)]

        def send_weights(c):
            for m in range(2):
                for d in range(1, n):
                    push(weight_from(m, row(d), c, r), weight_at(m, c, z, r),
                         send.at[wz, m, c], recv.at[wz, m, c], {"row": row(d)})

        def pass_weights(c):
            for m in range(2):
                wait(weight_bytes(m, c), recv.at[wz, m, c])
                for d in range(1, n):
                    at = weight_at(m, c, row(d), r)
                    push(at, at, send.at[wx, m, c], recv.at[wx, m, c], far_to)
                for d in range(1, n):
                    at = weight_at(m, c, row(d), r)
                    push(at, at, send.at[wc, m, c], recv.at[wc, m, c], core_to)

        def hand_weights(c):
            for m in range(2):
                wait(weight_bytes(m, c), recv.at[wx, m, c])
                for d in range(1, n):
                    at = weight_at(m, c, row(d), core * 2 + (1 - far))
                    push(at, at, send.at[wf, m, c], recv.at[wf, m, c], core_to)

        def block_at(full, b):
            return full.at[mine, span(b * block, block)]

        def other_at(full, b):
            return full.at[span((1 - y) * half, half), span(b * block, block)]

        ways = (
            (lambda s: z - s, lambda s: jnp.logical_and(z + 1 < n, z - s >= 0), 1,
             lambda s: z - 1 - s, lambda s: z - 1 - s >= 0),
            (lambda s: z + s, lambda s: jnp.logical_and(z >= 1, z + s < n), n - 1,
             lambda s: z + 1 + s, lambda s: z + 1 + s < n),
        )
        for s in range(n - 1):
            for m, (a, full) in enumerate(arrays):
                for w, (sent, sends, to, _, _) in enumerate(ways):

                    @pl.when(sends(s))
                    def _():
                        src = a.at[mine, :] if s == 0 else block_at(full, sent(s))
                        push(src, block_at(full, sent(s)), line_s.at[m, w, s], line_r.at[m, w, s],
                             {"row": row(to)})

            if s == 0:
                send_weights(0)
            for m, (a, full) in enumerate(arrays):
                for w, (_, _, _, taken, takes) in enumerate(ways):

                    @pl.when(takes(s))
                    def _():
                        at = block_at(full, taken(s))
                        wait(at, line_r.at[m, w, s])
                        push(at, at, y_s.at[m, w, s], y_r.at[m, w, s], y_to)

        for c in range(1, chunks):
            send_weights(c)
        pass_weights(0)
        for copy in own_loads:
            copy.wait()
        for s in range(n - 1):
            for m, (a, full) in enumerate(arrays):
                for w, (_, _, _, taken, takes) in enumerate(ways):

                    @pl.when(takes(s))
                    def _():
                        wait(other_at(full, taken(s)), y_r.at[m, w, s])

        def load_weights(c):
            for m in range(2):
                wait(weight_bytes(m, c), recv.at[wc, m, c])
                wait(weight_bytes(m, c), recv.at[wf, m, c])
            copies = []
            for d in range(n):
                b = span(row(d) * block, block)
                at = span((row(d) * chunks + c) * chunk, chunk)
                src_e = e_ref.at[:, at] if d == 0 else we_ref.at[c, b, :]
                src_t = t_ref.at[at, :] if d == 0 else wt_ref.at[c, :, b]
                copies.append(pltpu.make_async_copy(src_e, e_buf.at[b, :], loc.at[2 * d]))
                copies.append(pltpu.make_async_copy(src_t, t_buf.at[:, b], loc.at[2 * d + 1]))
            for copy in copies:
                copy.start()
            for copy in copies:
                copy.wait()

        def forward(c):
            load_weights(c)
            bias = bias_ref[:, c * chunk : (c + 1) * chunk]

            def step(t, total):
                at = span(t * token_tile, token_tile)
                pre = jnp.dot(x_all[at, :], e_buf[...], preferred_element_type=F32)
                v = (pre + bias).astype(BF16).astype(F32)
                back = dot(u_all[at, :], t_buf[...], 1, 1).astype(BF16).astype(F32)
                v2 = v * v
                th = jnp.tanh(c0 * (v + c1 * (v2 * v)))
                cdf = 0.5 * (1.0 + th)
                act[at, :] = (v * cdf).astype(BF16)
                slope = cdf + 0.5 * v * (1.0 - th * th) * (c0 * (1.0 + (3.0 * c1) * v2))
                g = (back * slope).astype(BF16)
                hg[c, at, :] = g
                return total + jnp.sum(g.astype(F32), axis=0, keepdims=True)

            total = lax.fori_loop(0, tokens // token_tile, step, jnp.zeros((1, chunk), F32))
            gb_ref[:, c * chunk : (c + 1) * chunk] = total * factor
            act_t[...] = act[...].T

        def free_slot(c):
            slot = c % 2
            for m, part in enumerate((pe, pt)):
                wait(part.at[slot, pl.ds(0, 2)], send.at[rc, m, c])
                wait(part.at[slot, 0], send.at[rx, m, c])
                wait(zbytes(m, part, slot), send.at[az, m, c])

        def zbytes(m, part, slot):
            if m == 0:
                return part.at[slot, 0, pl.ds(0, (n - 1) * block), :]
            return part.at[slot, 0, :, pl.ds(0, (n - 1) * block)]

        def grads(c):
            slot = c % 2

            def step_t(t, carry):
                at = span(t * model_tile, model_tile)
                g = (jnp.dot(act_t[...], u_all[:, at], preferred_element_type=F32) * factor).astype(BF16)
                for j in range(q):
                    pt[slot, j, :, at] = g[j * quarter : (j + 1) * quarter, :]
                return carry

            def step_e(t, carry):
                at = span(t * model_tile, model_tile)
                g = (dot(x_all[:, at], hg[c], 0, 0) * factor).astype(BF16)
                for j in range(q):
                    pe[slot, j, at, :] = g[:, j * quarter : (j + 1) * quarter]
                return carry

            other = pl.ds((1 - core) * 2, 2)
            lax.fori_loop(0, model // model_tile, step_t, 0)
            push(pt.at[slot, other], r1t_ref.at[c], send.at[rc, 1, c], recv.at[rc, 1, c], core_to)
            lax.fori_loop(0, model // model_tile, step_e, 0)
            push(pe.at[slot, other], r1e_ref.at[c], send.at[rc, 0, c], recv.at[rc, 0, c], core_to)

        def add_into(part, slot, j, got, tiles):
            rows = got.shape[0] // tiles

            def step(t, carry):
                at = span(t * rows, rows)
                total = part[slot, j, at, :].astype(F32) + got[at, :].astype(F32)
                part[slot, j, at, :] = total.astype(BF16)
                return carry

            lax.fori_loop(0, tiles, step, 0)

        sets = ((0, pe, tmp_e, r1e_ref, r2e_ref), (1, pt, tmp_t, r1t_ref, r2t_ref))

        def fold_core(c):
            slot = c % 2
            for m, part, tmp, r1, r2 in reversed(sets):
                wait(r1.at[c], recv.at[rc, m, c])
                copy = pltpu.make_async_copy(r1.at[c], tmp, loc.at[m])
                copy.start()
                copy.wait()
                for s in (1, 0):
                    h = (1 - far) if s else far
                    add_into(part, slot, core * 2 + h, tmp.at[h], 8)
                    if s:
                        push(part.at[slot, core * 2 + h], r2.at[c],
                             send.at[rx, m, c], recv.at[rx, m, c], far_to)

        def out_at(m, b, c, s):
            at = span(((b * chunks + c) * q + s) * quarter, quarter)
            return ge_ref.at[:, at] if m == 0 else gt_ref.at[at, :]

        def out_bytes(m, count):
            if m == 0:
                return ge_ref.at[:, pl.ds(0, count * quarter)]
            return gt_ref.at[pl.ds(0, count * quarter), :]

        def piece(m, part, slot, b):
            at = span(b * block, block)
            return part.at[slot, r, at, :] if m == 0 else part.at[slot, r, :, at]

        def fold_far(c):
            slot = c % 2
            for m, part, tmp, r1, r2 in reversed(sets):
                wait(r2.at[c], recv.at[rx, m, c])
                copy = pltpu.make_async_copy(r2.at[c], tmp.at[0], loc.at[m])
                copy.start()
                copy.wait()
                add_into(part, slot, r, tmp.at[0], 8)
                for d in range(1, n):
                    push(piece(m, part, slot, row(d)), out_at(m, z, c, r),
                         send.at[az, m, c], recv.at[az, m, c], {"row": row(d)})
                copy = pltpu.make_async_copy(piece(m, part, slot, z), out_at(m, z, c, r), loc.at[m])
                copy.start()
                copy.wait()

        def pass_grads(c):
            for m in (1, 0):
                wait(out_bytes(m, n - 1), recv.at[az, m, c])
                for d in range(n):
                    at = out_at(m, row(d), c, r)
                    push(at, at, send.at[ax, m, c], recv.at[ax, m, c], far_to)
                for d in range(n):
                    at = out_at(m, row(d), c, r)
                    push(at, at, send.at[ac, m, c], recv.at[ac, m, c], core_to)

        def hand_grads(c):
            for m in (1, 0):
                wait(out_bytes(m, n), recv.at[ax, m, c])
                for d in range(n):
                    at = out_at(m, row(d), c, core * 2 + (1 - far))
                    push(at, at, send.at[af, m, c], recv.at[af, m, c], core_to)

        def share_inputs():
            for d in range(n):
                b = row(d)
                for piece_at in range(block // model_tile):
                    first = pl.multiple_of(b * block + piece_at * model_tile, model_tile)
                    copies = []
                    for c in range(chunks):
                        if d == 0:
                            src = e_ref.at[pl.ds(piece_at * model_tile, model_tile),
                                           span((z * chunks + c) * chunk, chunk)]
                        else:
                            src = we_ref.at[c, pl.ds(first, model_tile), :]
                        copies.append(pltpu.make_async_copy(
                            src, e_buf.at[pl.ds(c * model_tile, model_tile), :], loc.at[c]))
                    for copy in copies:
                        copy.start()
                    for copy in copies:
                        copy.wait()

                    def step(t, carry):
                        at = span(t * token_tile, token_tile)
                        total = jnp.zeros((token_tile, model_tile), F32)
                        for c in range(chunks):
                            w = e_buf[c * model_tile : (c + 1) * model_tile, :]
                            total = total + dot(hg[c, at, :], w, 1, 1)
                        gx_all[at, pl.ds(first, model_tile)] = total.astype(BF16)
                        return carry

                    lax.fori_loop(0, tokens // token_tile, step, 0)
            theirs = span((1 - y) * half, half)
            push(gx_all.at[theirs, :], s1_ref, gi_s.at[0], gi_r.at[0], y_to)

        rows = half // 8

        def fold_col():
            wait(s1_ref, gi_r.at[0])
            copy = pltpu.make_async_copy(s1_ref, t_buf.at[pl.ds(0, half), :], loc.at[0])
            copy.start()
            copy.wait()

            def step(t, carry):
                at = pl.ds(pl.multiple_of(y * half + t * rows, rows), rows)
                total = gx_all[at, :].astype(F32) + t_buf[span(t * rows, rows), :].astype(F32)
                gx_all[at, :] = total.astype(BF16)
                return carry

            lax.fori_loop(0, 8, step, 0)
            for d in range(1, n):
                push(gx_all.at[mine, span(row(d) * block, block)], s2_ref.at[d - 1],
                     gi_s.at[1], gi_r.at[1], {"row": row(d)})

        def fold_row():
            wait(s2_ref, gi_r.at[1])
            copies = []
            for d in range(1, n):
                copies.append(pltpu.make_async_copy(
                    s2_ref.at[d - 1], t_buf.at[pl.ds(0, half), pl.ds((d - 1) * block, block)],
                    loc.at[d]))
            for copy in copies:
                copy.start()
            for copy in copies:
                copy.wait()
            at_z = span(z * block, block)

            def step(t, carry):
                at = pl.ds(pl.multiple_of(y * half + t * rows, rows), rows)
                here = span(t * rows, rows)
                total = gx_all[at, at_z].astype(F32)
                for d in range(1, n):
                    total = total + t_buf[here, pl.ds((d - 1) * block, block)].astype(F32)
                gx_all[at, at_z] = total.astype(BF16)
                return carry

            lax.fori_loop(0, 8, step, 0)
            src = gx_all.at[mine, at_z]
            push(src, gx_ref.at[mine, :], gi_s.at[2], gi_r.at[2], y_to)
            copy = pltpu.make_async_copy(src, gx_ref.at[mine, :], loc.at[0])
            copy.start()
            copy.wait()

        hand_weights(0)
        for c in range(chunks):
            if c + 1 < chunks:
                pass_weights(c + 1)
            forward(c)
            if c == chunks - 1:
                share_inputs()
            if c >= 2:
                free_slot(c - 2)
            grads(c)
            fold_core(c)
            if c + 1 < chunks:
                hand_weights(c + 1)
            if c >= 1:
                fold_far(c - 1)
            if c >= 2:
                pass_grads(c - 2)
            if c >= 3:
                hand_grads(c - 3)
        last = chunks - 1
        fold_col()
        fold_far(last)
        if last >= 1:
            pass_grads(last - 1)
        if last >= 2:
            hand_grads(last - 2)
        fold_row()
        pass_grads(last)
        if last >= 1:
            hand_grads(last - 1)
        hand_grads(last)

        for c in range(max(0, chunks - 2), chunks):
            free_slot(c)
        for c in range(chunks):
            for m in range(2):
                for stage in (wz, wx, wc, wf):
                    wait(weight_bytes(m, c), send.at[stage, m, c])
                for stage in (ax, ac, af):
                    wait(out_bytes(m, n), send.at[stage, m, c])
                for stage in (ac, af):
                    wait(out_bytes(m, n), recv.at[stage, m, c])
        wait(s1_ref, gi_s.at[0])
        wait(s2_ref, gi_s.at[1])
        wait(gx_ref.at[mine, :], gi_s.at[2])
        wait(gx_ref.at[mine, :], gi_r.at[2])
        for s in range(n - 1):
            for m, (a, full) in enumerate(arrays):
                for w, (sent, sends, _, taken, takes) in enumerate(ways):

                    @pl.when(sends(s))
                    def _():
                        wait(block_at(full, sent(s)), line_s.at[m, w, s])

                    @pl.when(takes(s))
                    def _():
                        wait(block_at(full, taken(s)), y_s.at[m, w, s])

    hbm = pl.BlockSpec(memory_space=pl.ANY)
    vmem = pl.BlockSpec(memory_space=pltpu.VMEM)
    z = lax.axis_index("row")
    own_bias = lax.dynamic_slice_in_dim(biases, z * own_width, own_width)[None]
    shaped = lambda *shape: jax.ShapeDtypeStruct(shape, BF16)
    dma = pltpu.SemaphoreType.DMA
    flops = 10 * tokens * model * own_width
    outs = pl.pallas_call(
        kernel,
        in_specs=[hbm, hbm, hbm, vmem, hbm],
        out_specs=[hbm, hbm, hbm, vmem] + [hbm] * 8,
        out_shape=[
            shaped(tokens, block),
            shaped(block, width),
            shaped(width, block),
            jax.ShapeDtypeStruct((1, own_width), F32),
            shaped(chunks, model, chunk),
            shaped(chunks, chunk, model),
            shaped(chunks, 2, model, quarter),
            shaped(chunks, 2, quarter, model),
            shaped(chunks, model, quarter),
            shaped(chunks, quarter, model),
            shaped(half, model),
            shaped(n - 1, half, block),
        ],
        scratch_shapes=[
            pltpu.VMEM((tokens, model), BF16),
            pltpu.VMEM((tokens, model), BF16),
            pltpu.VMEM((model, chunk), BF16),
            pltpu.VMEM((chunk, model), BF16),
            pltpu.VMEM((tokens, chunk), BF16),
            pltpu.VMEM((chunk, tokens), BF16),
            pltpu.VMEM((chunks, tokens, chunk), BF16),
            pltpu.VMEM((2, q, model, quarter), BF16),
            pltpu.VMEM((2, q, quarter, model), BF16),
            pltpu.VMEM((2, model, quarter), BF16),
            pltpu.VMEM((2, quarter, model), BF16),
            pltpu.VMEM((tokens, model), BF16),
            dma((2, 2, n - 1)),
            dma((2, 2, n - 1)),
            dma((2, 2, n - 1)),
            dma((2, 2, n - 1)),
            dma((10, 2, chunks)),
            dma((10, 2, chunks)),
            dma((3,)),
            dma((3,)),
            dma((2 * n,)),
        ],
        compiler_params=pltpu.CompilerParams(
            collective_id=0, has_side_effects=True, vmem_limit_bytes=67_000_000
        ),
        cost_estimate=pl.CostEstimate(flops=flops, bytes_accessed=200_000_000, transcendentals=0),
        name="fused",
    )(inputs, upstream, expand, own_bias, contract)
    grad_inputs, grad_expand, grad_contract, bias_part = outs[:4]

    vector = jnp.zeros((width + model,), F32)
    bias_part = bias_part[0].astype(BF16).astype(F32)
    vector = lax.dynamic_update_slice_in_dim(vector, bias_part, z * own_width, axis=0)
    offset = (jnp.sum(upstream, axis=0, dtype=F32) * factor).astype(BF16).astype(F32)
    vector = lax.dynamic_update_slice_in_dim(vector, offset, width + z * block, axis=0)
    vector = lax.psum(vector, ("row", "dp"))
    grad_biases = vector[:width].astype(BF16)
    grad_offset = lax.dynamic_slice_in_dim(vector, width + z * block, block, axis=0).astype(BF16)
    return (grad_inputs, grad_expand, grad_biases, grad_contract, grad_offset)


def program(inputs, upstream, expand, biases, contract):
    n, k, q = lax.axis_size("row"), lax.axis_size("col"), lax.axis_size("dp")
    tokens, block = inputs.shape
    own_width = expand.shape[1] // n
    fits = q == 4 and k == 2 and n > 1 and own_width % (q * LANES) == 0
    fits = fits and tokens % 512 == 0 and block % 512 == 0 and tokens // k <= q * LANES
    body = fused_local if fits else local
    return body(inputs, upstream, expand, biases, contract)


def solution(mesh):
    in_specs = (P("dp", "row"), P("dp", "row"), P("row", "col"), P("col"), P("col", "row"))
    out_specs = (P("dp", "row"), P("row", "col"), P("col"), P("col", "row"), P("row"))
    return jax.shard_map(program, mesh=mesh, in_specs=in_specs, out_specs=out_specs, check_vma=False)
```

```python
import functools

import jax
import jax.numpy as jnp
from jax import lax
from jax.experimental import pallas as pl
from jax.experimental.pallas import tpu as pltpu
from jax.sharding import PartitionSpec as P

LANES = 128
F32 = jnp.float32
BF16 = jnp.bfloat16


def gelu_tanh(values):
    return jax.nn.gelu(values, approximate=True)


def pointwise(hidden, backward):
    forward_act, pullback = jax.vjp(gelu_tanh, hidden.astype(F32))
    (slope_grad,) = pullback(backward.astype(F32))
    return (forward_act.astype(BF16), slope_grad.astype(BF16))


def swap(value, axis, distance):
    n = lax.axis_size(axis)
    return lax.ppermute(value, axis, [(i, i ^ distance) for i in range(n)])


def bits(axis):
    n = lax.axis_size(axis)
    assert n & (n - 1) == 0
    return [1 << b for b in range(n.bit_length() - 1)]


def dp_order():
    order = [0]
    for b in reversed(bits("dp")):
        order = order + [j ^ b for j in order]
    return order


def dot(a, b, ca, cb):
    return lax.dot_general(a, b, (((ca,), (cb,)), ((), ())), preferred_element_type=F32)


def pick(array, index, axis, width, sends):
    other = array.shape[1 - axis]
    total = index.shape[0]
    joined = total - sends
    if width % LANES:
        parts = [
            lax.dynamic_slice_in_dim(array, index[t] * width, width, axis=axis) for t in range(total)
        ]
        return parts[:sends] + [jnp.concatenate(parts[sends:], axis=axis)]
    steps = 4 if other % (4 * LANES) == 0 else 1
    size = other // steps

    def kernel(index_ref, *refs):
        ins, outs = refs[:total], refs[total:]
        for t in range(total):
            if t < sends:
                outs[t][...] = ins[t][...]
            else:
                at = pl.ds((t - sends) * width, width)
                if axis == 1:
                    outs[sends][:, at] = ins[t][...]
                else:
                    outs[sends][at, :] = ins[t][...]

    def spec(t):
        if axis == 1:
            return pl.BlockSpec((size, width), lambda g, idx: (g, idx[t]))
        return pl.BlockSpec((width, size), lambda g, idx: (idx[t], g))

    def out_spec(count):
        if axis == 1:
            return pl.BlockSpec((size, count * width), lambda g, idx: (g, 0))
        return pl.BlockSpec((count * width, size), lambda g, idx: (0, g))

    def out_type(count):
        shape = (other, count * width) if axis == 1 else (count * width, other)
        return jax.ShapeDtypeStruct(shape, array.dtype)

    counts = [1] * sends + [joined]
    moved = 2 * total * width * other * array.dtype.itemsize
    return pl.pallas_call(
        kernel,
        grid_spec=pltpu.PrefetchScalarGridSpec(
            num_scalar_prefetch=1,
            grid=(steps,),
            in_specs=[spec(t) for t in range(total)],
            out_specs=[out_spec(c) for c in counts],
        ),
        out_shape=[out_type(c) for c in counts],
        cost_estimate=pl.CostEstimate(flops=moved, bytes_accessed=moved, transcendentals=0),
        name="pick",
    )(index, *([array] * total))


def place(target, kept, got, index, axis, shape):
    half, n, rows, cols = kept.shape
    width = cols if axis == 1 else rows
    i = lax.axis_index("dp")
    odd = (i % 2).astype(jnp.int32)
    if axis == 1 and (2 * width) % LANES:
        target = jnp.zeros(shape, kept.dtype) if target is None else target
        first = jnp.where(odd == 0, kept, got)
        second = jnp.where(odd == 0, got, kept)
        for d in range(n):
            for p in range(half):
                pair = jnp.concatenate([first[p, d], second[p, d]], axis=axis)
                target = lax.dynamic_update_slice_in_dim(
                    target, pair, index[d * half + p] * 2 * width, axis=axis
                )
        return target

    def kernel(index_ref, *refs):
        a, b, out = refs[0], refs[1], refs[-1]
        is_odd = index_ref[n * half] == 1

        def put(lo, hi):
            if axis == 1:
                out[:, :width] = lo[0, 0]
                out[:, width:] = hi[0, 0]
            else:
                out[:width, :] = lo[0, 0]
                out[width:, :] = hi[0, 0]

        @pl.when(is_odd)
        def _():
            put(b, a)

        @pl.when(jnp.logical_not(is_odd))
        def _():
            put(a, b)

    spec = pl.BlockSpec((1, 1, rows, cols), lambda d, p, idx: (p, d, 0, 0))
    if axis == 1:
        out_spec = pl.BlockSpec((rows, 2 * width), lambda d, p, idx: (0, idx[d * half + p]))
    else:
        out_spec = pl.BlockSpec((2 * width, cols), lambda d, p, idx: (idx[d * half + p], 0))
    extra = [] if target is None else [target]
    moved = 2 * kept.size * 2 * kept.dtype.itemsize
    return pl.pallas_call(
        kernel,
        grid_spec=pltpu.PrefetchScalarGridSpec(
            num_scalar_prefetch=1,
            grid=(n, half),
            in_specs=[spec, spec] + [pl.BlockSpec(memory_space=pl.ANY)] * len(extra),
            out_specs=out_spec,
        ),
        out_shape=jax.ShapeDtypeStruct(shape, kept.dtype),
        input_output_aliases={3: 0} if extra else {},
        cost_estimate=pl.CostEstimate(flops=moved, bytes_accessed=moved, transcendentals=0),
        name="place",
    )(jnp.concatenate([index, odd[None]]), kept, got, *extra)


def gather_tokens(array):
    n, k = lax.axis_size("row"), lax.axis_size("col")
    y = lax.axis_index("col")
    piece = array.shape[0] // k
    pieces = [lax.dynamic_slice_in_dim(array, (y ^ e) * piece, piece, axis=0) for e in range(k)]
    rows = [[p] for p in pieces]
    for d in range(1, n):
        own = swap(pieces[0], "row", d)
        rows[0].append(own)
        for e in range(1, k):
            rows[e].append(swap(own, "col", e))
    return jnp.concatenate([jnp.concatenate(r, axis=1) for r in rows], axis=0)


def join_dp(part, axis):
    for b in reversed(bits("dp")):
        part = jnp.concatenate([part, swap(part, "dp", b)], axis=axis)
    return part


def reduce_dp(part, axis):
    for b in bits("dp"):
        half = part.shape[axis] // 2
        keep = lax.slice_in_dim(part, 0, half, axis=axis)
        got = swap(lax.slice_in_dim(part, half, 2 * half, axis=axis), "dp", b)
        part = (keep.astype(F32) + got.astype(F32)).astype(BF16)
    return part


def spread(part, axis):
    n = lax.axis_size("row")
    block = part.shape[1 - axis] // n
    cut = [lax.slice_in_dim(part, d * block, (d + 1) * block, axis=1 - axis) for d in range(n)]
    mine = jnp.stack([cut[0]] + [swap(cut[d], "row", d) for d in range(1, n)])[None]
    order = list(reversed(bits("dp")))
    for b in order[:-1]:
        mine = jnp.concatenate([mine, swap(mine, "dp", b)], axis=0)
    return mine, swap(mine, "dp", order[-1])


def local(inputs, upstream, expand, biases, contract):
    n, k, q = lax.axis_size("row"), lax.axis_size("col"), lax.axis_size("dp")
    z, y, i = lax.axis_index("row"), lax.axis_index("col"), lax.axis_index("dp")
    tokens, block = inputs.shape
    width = expand.shape[1]
    factor = (tokens * q) ** (-0.5)
    own_width = width // n
    chunks = max(1, own_width // (q * LANES))
    chunk = own_width // chunks
    quarter = chunk // q
    order = dp_order()

    inputs_all = gather_tokens(inputs)
    upstream_all = gather_tokens(upstream)

    def source(c):
        far = [((z ^ d) * chunks + c) * q + i for d in range(1, n)]
        near = [(z * chunks + c) * q + (i ^ j) for j in order]
        return jnp.stack(far + near).astype(jnp.int32)

    def goal(c):
        half = order[: q // 2]
        return jnp.stack(
            [(((z ^ d) * chunks + c) * q + (i ^ j)) // 2 for d in range(n) for j in half]
        ).astype(jnp.int32)

    bias_rows = []
    grad_expand = grad_contract = share = None
    for c in range(chunks):
        index = source(c)
        *far_e, near_e = pick(expand, index, 1, quarter, n - 1)
        *far_c, near_c = pick(contract, index, 0, quarter, n - 1)
        rest_e = jnp.concatenate([swap(far_e[d - 1], "row", d) for d in range(1, n)], axis=0)
        rest_c = jnp.concatenate([swap(far_c[d - 1], "row", d) for d in range(1, n)], axis=1)
        expand_c = jnp.concatenate([near_e, join_dp(rest_e, 1)], axis=0)
        contract_c = jnp.concatenate([near_c, join_dp(rest_c, 0)], axis=1)
        near = [lax.dynamic_slice_in_dim(biases, index[n - 1 + t] * quarter, quarter) for t in range(q)]
        pre = dot(inputs_all, expand_c, 1, 0)
        back = dot(upstream_all, contract_c, 1, 1).astype(BF16)
        hidden = (pre + jnp.concatenate(near)[None, :]).astype(BF16)
        active, grad = pointwise(hidden, back)
        contract_part = (dot(active, upstream_all, 0, 0) * factor).astype(BF16)
        expand_part = (dot(inputs_all, grad, 0, 0) * factor).astype(BF16)
        bias_rows.append((jnp.sum(grad, axis=0, dtype=F32) * factor).astype(BF16).astype(F32))
        kept, got = spread(reduce_dp(contract_part, 0), 0)
        grad_contract = place(grad_contract, kept, got, goal(c), 0, contract.shape)
        kept, got = spread(reduce_dp(expand_part, 1), 1)
        grad_expand = place(grad_expand, kept, got, goal(c), 1, expand.shape)
        term = dot(grad, expand_c, 1, 1)
        share = term if share is None else share + term

    piece = tokens // k
    share = share.astype(BF16)
    total = share[:piece].astype(F32)
    for e in range(1, k):
        total = total + swap(share[e * piece : (e + 1) * piece], "col", e).astype(F32)
    total = total.astype(BF16)
    mine = total[:, :block].astype(F32)
    for d in range(1, n):
        mine = mine + swap(total[:, d * block : (d + 1) * block], "row", d).astype(F32)
    mine = mine.astype(BF16)
    grad_inputs = jnp.zeros((tokens, block), BF16)
    for e in range(k):
        got = mine if e == 0 else swap(mine, "col", e)
        grad_inputs = lax.dynamic_update_slice_in_dim(grad_inputs, got, (y ^ e) * piece, axis=0)

    vector = jnp.zeros((width + n * block,), F32)
    for c in range(chunks):
        for t, j in enumerate(order):
            at = (((z * chunks + c) * q) + (i ^ j)) * quarter
            vector = lax.dynamic_update_slice_in_dim(
                vector, bias_rows[c][t * quarter : (t + 1) * quarter], at, axis=0
            )
    offset = (jnp.sum(upstream, axis=0, dtype=F32) * factor).astype(BF16).astype(F32)
    vector = lax.dynamic_update_slice_in_dim(vector, offset, width + z * block, axis=0)
    vector = lax.psum(vector, ("row", "dp"))
    grad_biases = vector[:width].astype(BF16)
    grad_offset = lax.dynamic_slice_in_dim(vector, width + z * block, block, axis=0).astype(BF16)
    return (grad_inputs, grad_expand, grad_biases, grad_contract, grad_offset)


def fused_local(inputs, upstream, expand, biases, contract):
    n, k, q = lax.axis_size("row"), lax.axis_size("col"), lax.axis_size("dp")
    tokens, block = inputs.shape
    model = n * block
    width = expand.shape[1]
    own_width = width // n
    quarter = LANES
    chunk = q * quarter
    chunks = own_width // chunk
    half = tokens // k
    slots = 4
    parts = 2
    factor = (tokens * q) ** (-0.5)
    c0 = 0.7978845608028654
    c1 = 0.044715
    token_tile = 256 if tokens % 256 == 0 else tokens
    model_tile = 512 if block % 512 == 0 else block

    def kernel(
        x_ref, u_ref, e_ref, bias_ref, t_ref,
        gx_ref, ge_ref, gt_ref, gb_ref, go_ref,
        we_ref, wt_ref, r1e_ref, r1t_ref, r2e_ref, r2t_ref, s1_ref, s2_ref,
        x_all, u_all, e_buf, t_buf, act_t, hg, pe, pt, vecs, vecs_in, bias_all,
        line_s, line_r, y_s, y_r, send, recv, gy_s, gy_r, gi_s, gi_r, vec_s, vec_r, loc,
    ):
        z, y, i = lax.axis_index("row"), lax.axis_index("col"), lax.axis_index("dp")
        core, far = lax.rem(i, 2), lax.div(i, 2)
        r = core * 2 + far
        core_to = {"dp": far * 2 + (1 - core)}
        far_to = {"dp": (1 - far) * 2 + core}
        y_to = {"col": 1 - y}

        def row(d):
            return lax.rem(z + d, n)

        def span(start, size):
            return pl.ds(pl.multiple_of(start, size), size)

        def push(src, dst, ss, rs, to):
            pltpu.make_async_remote_copy(
                src_ref=src, dst_ref=dst, send_sem=ss, recv_sem=rs,
                device_id=to, device_id_type=pl.DeviceIdType.MESH,
            ).start()

        def wait(region, sem):
            pltpu.make_async_copy(region, region, sem).wait()

        barrier = pltpu.get_barrier_semaphore()
        partners = [{"row": row(d)} for d in range(1, n)] + [y_to, core_to, far_to]
        for to in partners:
            pl.semaphore_signal(barrier, inc=1, device_id=to, device_id_type=pl.DeviceIdType.MESH)
        pl.semaphore_wait(barrier, len(partners))

        arrays = ((x_ref, x_all), (u_ref, u_all))
        mine = span(y * half, half)
        own_loads = [
            pltpu.make_async_copy(a, full.at[:, span(z * block, block)], loc.at[m])
            for m, (a, full) in enumerate(arrays)
        ]
        for copy in own_loads:
            copy.start()

        wz, wx, wc, wf, rc, rx, az, ax, ac, af = range(10)

        def direct(c):
            return c >= 1 and c == chunks - 1

        def wide(c):
            return 2 * quarter if direct(c) else quarter

        def first(c):
            return core * 2 if direct(c) else r

        def weight_at(m, c, b, s):
            at = pl.ds(pl.multiple_of(s * quarter, quarter), wide(c))
            if m == 0:
                return we_ref.at[c, span(b * block, block), at]
            return wt_ref.at[c, at, span(b * block, block)]

        def weight_from(m, b, c):
            at = ((b * chunks + c) * q + first(c)) * quarter
            at = pl.ds(pl.multiple_of(at, quarter), wide(c))
            return e_ref.at[:, at] if m == 0 else t_ref.at[at, :]

        def weight_bytes(m, c):
            if m == 0:
                return we_ref.at[c, pl.ds(0, (n - 1) * block), pl.ds(0, wide(c))]
            return wt_ref.at[c, pl.ds(0, wide(c)), pl.ds(0, (n - 1) * block)]

        def send_weights(c, m):
            for d in range(1, n):
                push(weight_from(m, row(d), c), weight_at(m, c, z, first(c)),
                     send.at[wz, m, c], recv.at[wz, m, c], {"row": row(d)})

        def pass_weights(c, m):
            wait(weight_bytes(m, c), recv.at[wz, m, c])
            for stage, to in ((wx, far_to), (wc, core_to)):
                if stage == wx and direct(c):
                    continue
                for d in range(1, n):
                    at = weight_at(m, c, row(d), first(c))
                    push(at, at, send.at[stage, m, c], recv.at[stage, m, c], to)

        def hand_weights(c, m):
            if direct(c):
                return
            wait(weight_bytes(m, c), recv.at[wx, m, c])
            for d in range(1, n):
                at = weight_at(m, c, row(d), core * 2 + (1 - far))
                push(at, at, send.at[wf, m, c], recv.at[wf, m, c], core_to)

        part = half // parts

        def block_at(full, b, h):
            return full.at[span(y * half + h * part, part), span(b * block, block)]

        def other_at(full, b, h):
            return full.at[span((1 - y) * half + h * part, part), span(b * block, block)]

        ways = (
            (lambda s: z - s, lambda s: jnp.logical_and(z + 1 < n, z - s >= 0), 1,
             lambda s: z - 1 - s, lambda s: z - 1 - s >= 0),
            (lambda s: z + s, lambda s: jnp.logical_and(z >= 1, z + s < n), n - 1,
             lambda s: z + 1 + s, lambda s: z + 1 + s < n),
        )
        def line_send(m, s, h, w, src):
            sent, _, to, _, _ = ways[w]
            at = block_at(arrays[m][1], sent(s), h)
            push(at if src is None else src, at, line_s.at[m, w, s, h], line_r.at[m, w, s, h],
                 {"row": row(to)})

        def line_start(m):
            for h in range(parts):
                for w in range(2):

                    @pl.when(ways[w][1](0))
                    def _():
                        rows_at = span(y * half + h * part, part)
                        line_send(m, 0, h, w, arrays[m][0].at[rows_at, :])

        def line_take(m, s):
            for h in range(parts):
                for w, (_, sends, _, taken, takes) in enumerate(ways):

                    @pl.when(takes(s))
                    def _():
                        at = block_at(arrays[m][1], taken(s), h)
                        wait(at, line_r.at[m, w, s, h])
                        if s < n - 2:

                            @pl.when(sends(s + 1))
                            def _():
                                line_send(m, s + 1, h, w, None)

                        push(at, at, y_s.at[m, w, s, h], y_r.at[m, w, s, h], y_to)

        def line_join(m):
            for s in range(n - 1):
                for w, (_, _, _, taken, takes) in enumerate(ways):

                    @pl.when(takes(s))
                    def _():
                        for h in range(parts):
                            wait(other_at(arrays[m][1], taken(s), h), y_r.at[m, w, s, h])

        def line_end(m):
            full = arrays[m][1]
            for s in range(n - 1):
                for w, (sent, sends, _, taken, takes) in enumerate(ways):

                    @pl.when(sends(s))
                    def _():
                        for h in range(parts):
                            wait(block_at(full, sent(s), h), line_s.at[m, w, s, h])

                    @pl.when(takes(s))
                    def _():
                        for h in range(parts):
                            wait(block_at(full, taken(s), h), y_s.at[m, w, s, h])

        def load_weights(c, m):
            wait(weight_bytes(m, c), recv.at[wc, m, c])
            if not direct(c):
                wait(weight_bytes(m, c), recv.at[wf, m, c])
            copies = []
            for d in range(n):
                b = span(row(d) * block, block)
                at = span((row(d) * chunks + c) * chunk, chunk)
                if m == 0:
                    src = e_ref.at[:, at] if d == 0 else we_ref.at[c, b, :]
                    dst = e_buf.at[b, :]
                else:
                    src = t_ref.at[at, :] if d == 0 else wt_ref.at[c, :, b]
                    dst = t_buf.at[:, b]
                copies.append(pltpu.make_async_copy(src, dst, loc.at[d]))
            for copy in copies:
                copy.start()
            for copy in copies:
                copy.wait()

        def tanh_of(v, v2):
            return jnp.tanh(c0 * (v + c1 * (v2 * v)))

        def forward(c):
            load_weights(c, 0)
            bias = bias_ref[:, c * chunk : (c + 1) * chunk]

            def step(t, carry):
                at = span(t * token_tile, token_tile)
                pre = jnp.dot(x_all[at, :], e_buf[...], preferred_element_type=F32)
                hidden = (pre + bias).astype(BF16)
                hg[c, at, :] = hidden
                v = hidden.astype(F32)
                active = (0.5 * v * (1.0 + tanh_of(v, v * v))).astype(BF16)
                act_t[:, at] = active.T
                return carry

            lax.fori_loop(0, tokens // token_tile, step, 0)

        def backward(c):
            load_weights(c, 1)

            def step(t, total):
                at = span(t * token_tile, token_tile)
                back = dot(u_all[at, :], t_buf[...], 1, 1).astype(BF16).astype(F32)
                v = hg[c, at, :].astype(F32)
                v2 = v * v
                th = tanh_of(v, v2)
                slope = 0.5 * (1.0 + th) + 0.5 * v * (1.0 - th * th) * (c0 * (1.0 + (3.0 * c1) * v2))
                g = (back * slope).astype(BF16)
                hg[c, at, :] = g
                return total + jnp.sum(g.astype(F32), axis=0, keepdims=True)

            total = lax.fori_loop(0, tokens // token_tile, step, jnp.zeros((1, chunk), F32))
            vecs[0, :, c * chunk : (c + 1) * chunk] = (total * factor).astype(BF16).astype(F32)

        def offset():
            def step(t, total):
                at = span(t * token_tile, token_tile)
                part = u_all[at, span(z * block, block)].astype(F32)
                return total + jnp.sum(part, axis=0, keepdims=True)

            total = lax.fori_loop(0, tokens // token_tile, step, jnp.zeros((1, block), F32))
            vecs[0, :, own_width:] = (total * factor).astype(BF16).astype(F32)

        def bias_core():
            push(vecs.at[0], vecs_in.at[0], vec_s.at[0], vec_r.at[0], core_to)

        def bias_far():
            wait(vecs_in.at[0], vec_r.at[0])
            vecs[1] = vecs[0] + vecs_in[0]
            push(vecs.at[1], vecs_in.at[1], vec_s.at[1], vec_r.at[1], far_to)

        def bias_row():
            wait(vecs_in.at[1], vec_r.at[1])
            vecs[2] = vecs[1] + vecs_in[1]
            for d in range(1, n):
                push(vecs.at[2, :, pl.ds(0, own_width)], bias_all.at[z],
                     vec_s.at[2], vec_r.at[2], {"row": row(d)})
            bias_all[z] = vecs[2, :, :own_width]

        def bias_end():
            wait(bias_all.at[pl.ds(0, n - 1)], vec_r.at[2])
            gb_ref[...] = bias_all[...].astype(BF16)
            go_ref[...] = vecs[2, :, own_width:].astype(BF16)
            wait(bias_all.at[pl.ds(0, n - 1)], vec_s.at[2])
            wait(vecs.at[0], vec_s.at[0])
            wait(vecs.at[1], vec_s.at[1])

        def free_slot(c):
            slot = c % slots
            for m, part in enumerate((pe, pt)):
                wait(part.at[slot, pl.ds(0, 2)], send.at[rc, m, c])
                wait(part.at[slot, 0], send.at[rx, m, c])
                wait(zbytes(m, part, slot), send.at[az, m, c])

        def zbytes(m, part, slot):
            if m == 0:
                return part.at[slot, 0, pl.ds(0, (n - 1) * block), :]
            return part.at[slot, 0, :, pl.ds(0, (n - 1) * block)]

        other = pl.ds((1 - core) * 2, 2)

        def grads_t(c):
            slot = c % slots

            def step(t, carry):
                at = span(t * model_tile, model_tile)
                g = (jnp.dot(act_t[...], u_all[:, at], preferred_element_type=F32) * factor).astype(BF16)
                for j in range(q):
                    pt[slot, j, :, at] = g[j * quarter : (j + 1) * quarter, :]
                return carry

            lax.fori_loop(0, model // model_tile, step, 0)
            push(pt.at[slot, other], r1t_ref.at[c], send.at[rc, 1, c], recv.at[rc, 1, c], core_to)

        def grads_e(c):
            slot = c % slots

            def step(t, carry):
                at = span(t * model_tile, model_tile)
                g = (dot(x_all[:, at], hg[c], 0, 0) * factor).astype(BF16)
                for j in range(q):
                    pe[slot, j, at, :] = g[:, j * quarter : (j + 1) * quarter]
                return carry

            lax.fori_loop(0, model // model_tile, step, 0)
            push(pe.at[slot, other], r1e_ref.at[c], send.at[rc, 0, c], recv.at[rc, 0, c], core_to)

        def add_into(part, slot, j, got, tiles):
            rows = got.shape[0] // tiles

            def step(t, carry):
                at = span(t * rows, rows)
                total = part[slot, j, at, :].astype(F32) + got[at, :].astype(F32)
                part[slot, j, at, :] = total.astype(BF16)
                return carry

            lax.fori_loop(0, tiles, step, 0)

        sets = (
            (0, pe, [e_buf.at[:, pl.ds(h * quarter, quarter)] for h in range(2)], r1e_ref, r2e_ref),
            (1, pt, [t_buf.at[pl.ds(h * quarter, quarter), :] for h in range(2)], r1t_ref, r2t_ref),
        )

        def fetch(pairs):
            copies = [
                pltpu.make_async_copy(src, dst, loc.at[t]) for t, (src, dst) in enumerate(pairs)
            ]
            for copy in copies:
                copy.start()
            for copy in copies:
                copy.wait()


        def fold_core(c, which):
            slot = c % slots
            m, part, tmp, r1, r2 = sets[which]
            wait(r1.at[c], recv.at[rc, m, c])
            theirs = core * 2 + (1 - far)
            fetch([(r1.at[c, 1 - far], tmp[0]), (r1.at[c, far], tmp[1])])
            add_into(part, slot, theirs, tmp[0], 8)
            push(part.at[slot, theirs], r2.at[c], send.at[rx, m, c], recv.at[rx, m, c], far_to)
            add_into(part, slot, r, tmp[1], 8)

        def out_at(m, b, c, s):
            at = span(((b * chunks + c) * q + s) * quarter, quarter)
            return ge_ref.at[:, at] if m == 0 else gt_ref.at[at, :]

        def out_bytes(m, count):
            if m == 0:
                return ge_ref.at[:, pl.ds(0, count * quarter)]
            return gt_ref.at[pl.ds(0, count * quarter), :]

        def piece(m, part, slot, b):
            at = span(b * block, block)
            return part.at[slot, r, at, :] if m == 0 else part.at[slot, r, :, at]

        def fold_far(c, which):
            slot = c % slots
            m, part, tmp, r1, r2 = sets[which]
            wait(r2.at[c], recv.at[rx, m, c])
            fetch([(r2.at[c], tmp[0])])
            add_into(part, slot, r, tmp[0], 8)
            for d in range(1, n):
                push(piece(m, part, slot, row(d)), out_at(m, z, c, r),
                     send.at[az, m, c], recv.at[az, m, c], {"row": row(d)})
            copy = pltpu.make_async_copy(piece(m, part, slot, z), out_at(m, z, c, r), loc.at[0])
            copy.start()
            copy.wait()

        def pass_grads(c):
            for m in (1, 0):
                wait(out_bytes(m, n - 1), recv.at[az, m, c])
                for stage, to in ((ax, far_to), (ac, core_to)):
                    for d in range(n):
                        at = out_at(m, row(d), c, r)
                        push(at, at, send.at[stage, m, c], recv.at[stage, m, c], to)

        def hand_grads(c):
            for m in (1, 0):
                wait(out_bytes(m, n), recv.at[ax, m, c])
                for d in range(n):
                    at = out_at(m, row(d), c, core * 2 + (1 - far))
                    push(at, at, send.at[af, m, c], recv.at[af, m, c], core_to)

        theirs = span((1 - y) * half, half)

        def share_inputs(d):
            b = row(d)
            for piece_at in range(block // model_tile):
                start = pl.multiple_of(b * block + piece_at * model_tile, model_tile)
                copies = []
                for c in range(chunks):
                    if d == 0:
                        src = e_ref.at[pl.ds(piece_at * model_tile, model_tile),
                                       span((z * chunks + c) * chunk, chunk)]
                    else:
                        src = we_ref.at[c, pl.ds(start, model_tile), :]
                    copies.append(pltpu.make_async_copy(
                        src, e_buf.at[pl.ds(c * model_tile, model_tile), :], loc.at[c]))
                for copy in copies:
                    copy.start()
                for copy in copies:
                    copy.wait()

                def step(t, carry):
                    at = span(t * token_tile, token_tile)
                    total = jnp.zeros((token_tile, model_tile), F32)
                    for c in range(chunks):
                        w = e_buf[c * model_tile : (c + 1) * model_tile, :]
                        total = total + dot(hg[c, at, :], w, 1, 1)
                    x_all[at, pl.ds(start, model_tile)] = total.astype(BF16)
                    return carry

                lax.fori_loop(0, tokens // token_tile, step, 0)
            push(x_all.at[theirs, span(b * block, block)], s1_ref.at[d], gy_s.at[d], gy_r.at[d], y_to)

        rows = half // 8

        def fold_col(d):
            wait(s1_ref.at[d], gy_r.at[d])
            at_b = span(row(d) * block, block)
            got = t_buf.at[pl.ds(0, half), pl.ds(d * block, block)]
            copy = pltpu.make_async_copy(s1_ref.at[d], got, loc.at[0])
            copy.start()
            copy.wait()

            def step(t, carry):
                at = pl.ds(pl.multiple_of(y * half + t * rows, rows), rows)
                here = span(t * rows, rows)
                total = x_all[at, at_b].astype(F32) + got[here, :].astype(F32)
                x_all[at, at_b] = total.astype(BF16)
                return carry

            lax.fori_loop(0, 8, step, 0)
            if d > 0:
                push(x_all.at[mine, at_b], s2_ref.at[d - 1], gi_s.at[0], gi_r.at[0], {"row": row(d)})

        def fold_row():
            wait(s2_ref, gi_r.at[0])
            copies = []
            for d in range(1, n):
                copies.append(pltpu.make_async_copy(
                    s2_ref.at[d - 1], t_buf.at[pl.ds(0, half), pl.ds((d - 1) * block, block)],
                    loc.at[d]))
            for copy in copies:
                copy.start()
            for copy in copies:
                copy.wait()
            at_z = span(z * block, block)

            def step(t, carry):
                at = pl.ds(pl.multiple_of(y * half + t * rows, rows), rows)
                here = span(t * rows, rows)
                total = x_all[at, at_z].astype(F32)
                for d in range(1, n):
                    total = total + t_buf[here, pl.ds((d - 1) * block, block)].astype(F32)
                x_all[at, at_z] = total.astype(BF16)
                return carry

            lax.fori_loop(0, 8, step, 0)
            src = x_all.at[mine, at_z]
            push(src, gx_ref.at[mine, :], gi_s.at[1], gi_r.at[1], y_to)
            copy = pltpu.make_async_copy(src, gx_ref.at[mine, :], loc.at[0])
            copy.start()
            copy.wait()

        last = chunks - 1
        edge = n - 2

        line_start(0)
        send_weights(0, 0)
        for s in range(n - 1):
            if s == edge:
                line_start(1)
            line_take(0, s)
            if s == 0:
                pass_weights(0, 0)
        hand_weights(0, 0)
        for copy in own_loads:
            copy.wait()
        at_end = jnp.logical_or(z == 0, z == n - 1)
        for s in range(n - 1):
            if s == min(1, edge):
                line_join(0)
                forward(0)
                offset()
            line_take(1, s)
            if s == 0:

                @pl.when(at_end)
                def _():
                    send_weights(0, 1)

        line_join(1)

        @pl.when(jnp.logical_not(at_end))
        def _():
            send_weights(0, 1)

        for m in range(2):
            if chunks > 1:
                send_weights(1, m)

        for c in range(chunks):
            if c > 0:
                forward(c)
            if c >= slots:
                free_slot(c - slots)
            grads_t(c)
            if c == 0:
                pass_weights(0, 1)
                fold_core(0, 1)
                for later in range(2, chunks):
                    for m in range(2):
                        send_weights(later, m)
                hand_weights(0, 1)
            backward(c)
            if c > 0:
                fold_core(c, 1)
            if c + 1 < chunks and c >= 2:
                pass_weights(c + 1, 1)
            if c >= 3:
                pass_grads(c - 3)
            grads_e(c)
            if c == 0 and chunks > 1:
                pass_weights(1, 0)
                pass_weights(1, 1)
            if c == last:
                bias_core()
            fold_core(c, 0)
            if c + 1 < chunks:
                hand_weights(c + 1, 0)
                hand_weights(c + 1, 1)
            if c + 2 < chunks:
                pass_weights(c + 2, 0)
                if c == 0:
                    pass_weights(c + 2, 1)
            if c >= 1:
                fold_far(c - 1, 1)
                fold_far(c - 1, 0)
        done = max(0, last - 2)
        handed = 0
        bias_far()
        line_end(0)
        for d in range(1, n):
            if d == 1 and done < last - 1:
                pass_grads(done)
                done += 1
            share_inputs(d)
        share_inputs(0)
        fold_col(1)
        if done < last:
            pass_grads(done)
            done += 1
        fold_far(last, 1)
        fold_far(last, 0)
        for d in list(range(2, n)) + [0]:
            fold_col(d)
        for c in range(last - 1):
            hand_grads(c)
        while done <= last:
            pass_grads(done)
            done += 1
        fold_row()
        bias_row()
        for c in range(max(0, last - 1), chunks):
            hand_grads(c)
        bias_end()

        for c in range(max(0, chunks - slots), chunks):
            free_slot(c)
        for c in range(chunks):
            for m in range(2):
                for stage in (wz, wc) if direct(c) else (wz, wx, wc, wf):
                    wait(weight_bytes(m, c), send.at[stage, m, c])
                for stage in (ax, ac, af):
                    wait(out_bytes(m, n), send.at[stage, m, c])
                for stage in (ac, af):
                    wait(out_bytes(m, n), recv.at[stage, m, c])
        for d in range(n):
            wait(s1_ref.at[d], gy_s.at[d])
        wait(s2_ref, gi_s.at[0])
        wait(gx_ref.at[mine, :], gi_s.at[1])
        wait(gx_ref.at[mine, :], gi_r.at[1])
        line_end(1)

    hbm = pl.BlockSpec(memory_space=pl.ANY)
    vmem = pl.BlockSpec(memory_space=pltpu.VMEM)
    z = lax.axis_index("row")
    own_bias = lax.dynamic_slice_in_dim(biases, z * own_width, own_width)[None]
    shaped = lambda *shape: jax.ShapeDtypeStruct(shape, BF16)
    dma = pltpu.SemaphoreType.DMA
    flops = 10 * tokens * model * own_width
    outs = pl.pallas_call(
        kernel,
        in_specs=[hbm, hbm, hbm, vmem, hbm],
        out_specs=[hbm, hbm, hbm, vmem, vmem] + [hbm] * 8,
        out_shape=[
            shaped(tokens, block),
            shaped(block, width),
            shaped(width, block),
            shaped(n, 1, own_width),
            shaped(1, block),
            shaped(chunks, model, chunk),
            shaped(chunks, chunk, model),
            shaped(chunks, 2, model, quarter),
            shaped(chunks, 2, quarter, model),
            shaped(chunks, model, quarter),
            shaped(chunks, quarter, model),
            shaped(n, half, block),
            shaped(n - 1, half, block),
        ],
        scratch_shapes=[
            pltpu.VMEM((tokens, model), BF16),
            pltpu.VMEM((tokens, model), BF16),
            pltpu.VMEM((model, chunk), BF16),
            pltpu.VMEM((chunk, model), BF16),
            pltpu.VMEM((chunk, tokens), BF16),
            pltpu.VMEM((chunks, tokens, chunk), BF16),
            pltpu.VMEM((slots, q, model, quarter), BF16),
            pltpu.VMEM((slots, q, quarter, model), BF16),
            pltpu.VMEM((3, 1, own_width + block), F32),
            pltpu.VMEM((2, 1, own_width + block), F32),
            pltpu.VMEM((n, 1, own_width), F32),
            dma((2, 2, n - 1, parts)),
            dma((2, 2, n - 1, parts)),
            dma((2, 2, n - 1, parts)),
            dma((2, 2, n - 1, parts)),
            dma((10, 2, chunks)),
            dma((10, 2, chunks)),
            dma((n,)),
            dma((n,)),
            dma((2,)),
            dma((2,)),
            dma((3,)),
            dma((3,)),
            dma((max(n, chunks),)),
        ],
        compiler_params=pltpu.CompilerParams(
            collective_id=0, has_side_effects=True, vmem_limit_bytes=67_000_000
        ),
        cost_estimate=pl.CostEstimate(flops=flops, bytes_accessed=200_000_000, transcendentals=0),
        name="fused",
    )(inputs, upstream, expand, own_bias, contract)
    grad_inputs, grad_expand, grad_contract, grad_biases, grad_offset = outs[:5]
    return (
        grad_inputs,
        grad_expand,
        grad_biases.reshape(width),
        grad_contract,
        grad_offset.reshape(block),
    )


def program(inputs, upstream, expand, biases, contract):
    n, k, q = lax.axis_size("row"), lax.axis_size("col"), lax.axis_size("dp")
    tokens, block = inputs.shape
    own_width = expand.shape[1] // n
    fits = q == 4 and k == 2 and n > 1 and own_width % (q * LANES) == 0
    fits = fits and tokens % 512 == 0 and block % 512 == 0 and tokens // k <= q * LANES
    body = fused_local if fits else local
    return body(inputs, upstream, expand, biases, contract)


def solution(mesh):
    in_specs = (P("dp", "row"), P("dp", "row"), P("row", "col"), P("col"), P("col", "row"))
    out_specs = (P("dp", "row"), P("row", "col"), P("col"), P("col", "row"), P("row"))
    return jax.shard_map(program, mesh=mesh, in_specs=in_specs, out_specs=out_specs, check_vma=False)
```

```python
import functools

import jax
import jax.numpy as jnp
from jax import lax
from jax.experimental import pallas as pl
from jax.experimental.pallas import tpu as pltpu
from jax.sharding import PartitionSpec as P

LANES = 128
F32 = jnp.float32
BF16 = jnp.bfloat16


def gelu_tanh(values):
    return jax.nn.gelu(values, approximate=True)


def pointwise(hidden, backward):
    forward_act, pullback = jax.vjp(gelu_tanh, hidden.astype(F32))
    (slope_grad,) = pullback(backward.astype(F32))
    return (forward_act.astype(BF16), slope_grad.astype(BF16))


def swap(value, axis, distance):
    n = lax.axis_size(axis)
    return lax.ppermute(value, axis, [(i, i ^ distance) for i in range(n)])


def bits(axis):
    n = lax.axis_size(axis)
    assert n & (n - 1) == 0
    return [1 << b for b in range(n.bit_length() - 1)]


def dp_order():
    order = [0]
    for b in reversed(bits("dp")):
        order = order + [j ^ b for j in order]
    return order


def dot(a, b, ca, cb):
    return lax.dot_general(a, b, (((ca,), (cb,)), ((), ())), preferred_element_type=F32)


def pick(array, index, axis, width, sends):
    other = array.shape[1 - axis]
    total = index.shape[0]
    joined = total - sends
    if width % LANES:
        parts = [
            lax.dynamic_slice_in_dim(array, index[t] * width, width, axis=axis) for t in range(total)
        ]
        return parts[:sends] + [jnp.concatenate(parts[sends:], axis=axis)]
    steps = 4 if other % (4 * LANES) == 0 else 1
    size = other // steps

    def kernel(index_ref, *refs):
        ins, outs = refs[:total], refs[total:]
        for t in range(total):
            if t < sends:
                outs[t][...] = ins[t][...]
            else:
                at = pl.ds((t - sends) * width, width)
                if axis == 1:
                    outs[sends][:, at] = ins[t][...]
                else:
                    outs[sends][at, :] = ins[t][...]

    def spec(t):
        if axis == 1:
            return pl.BlockSpec((size, width), lambda g, idx: (g, idx[t]))
        return pl.BlockSpec((width, size), lambda g, idx: (idx[t], g))

    def out_spec(count):
        if axis == 1:
            return pl.BlockSpec((size, count * width), lambda g, idx: (g, 0))
        return pl.BlockSpec((count * width, size), lambda g, idx: (0, g))

    def out_type(count):
        shape = (other, count * width) if axis == 1 else (count * width, other)
        return jax.ShapeDtypeStruct(shape, array.dtype)

    counts = [1] * sends + [joined]
    moved = 2 * total * width * other * array.dtype.itemsize
    return pl.pallas_call(
        kernel,
        grid_spec=pltpu.PrefetchScalarGridSpec(
            num_scalar_prefetch=1,
            grid=(steps,),
            in_specs=[spec(t) for t in range(total)],
            out_specs=[out_spec(c) for c in counts],
        ),
        out_shape=[out_type(c) for c in counts],
        cost_estimate=pl.CostEstimate(flops=moved, bytes_accessed=moved, transcendentals=0),
        name="pick",
    )(index, *([array] * total))


def place(target, kept, got, index, axis, shape):
    half, n, rows, cols = kept.shape
    width = cols if axis == 1 else rows
    i = lax.axis_index("dp")
    odd = (i % 2).astype(jnp.int32)
    if axis == 1 and (2 * width) % LANES:
        target = jnp.zeros(shape, kept.dtype) if target is None else target
        first = jnp.where(odd == 0, kept, got)
        second = jnp.where(odd == 0, got, kept)
        for d in range(n):
            for p in range(half):
                pair = jnp.concatenate([first[p, d], second[p, d]], axis=axis)
                target = lax.dynamic_update_slice_in_dim(
                    target, pair, index[d * half + p] * 2 * width, axis=axis
                )
        return target

    def kernel(index_ref, *refs):
        a, b, out = refs[0], refs[1], refs[-1]
        is_odd = index_ref[n * half] == 1

        def put(lo, hi):
            if axis == 1:
                out[:, :width] = lo[0, 0]
                out[:, width:] = hi[0, 0]
            else:
                out[:width, :] = lo[0, 0]
                out[width:, :] = hi[0, 0]

        @pl.when(is_odd)
        def _():
            put(b, a)

        @pl.when(jnp.logical_not(is_odd))
        def _():
            put(a, b)

    spec = pl.BlockSpec((1, 1, rows, cols), lambda d, p, idx: (p, d, 0, 0))
    if axis == 1:
        out_spec = pl.BlockSpec((rows, 2 * width), lambda d, p, idx: (0, idx[d * half + p]))
    else:
        out_spec = pl.BlockSpec((2 * width, cols), lambda d, p, idx: (idx[d * half + p], 0))
    extra = [] if target is None else [target]
    moved = 2 * kept.size * 2 * kept.dtype.itemsize
    return pl.pallas_call(
        kernel,
        grid_spec=pltpu.PrefetchScalarGridSpec(
            num_scalar_prefetch=1,
            grid=(n, half),
            in_specs=[spec, spec] + [pl.BlockSpec(memory_space=pl.ANY)] * len(extra),
            out_specs=out_spec,
        ),
        out_shape=jax.ShapeDtypeStruct(shape, kept.dtype),
        input_output_aliases={3: 0} if extra else {},
        cost_estimate=pl.CostEstimate(flops=moved, bytes_accessed=moved, transcendentals=0),
        name="place",
    )(jnp.concatenate([index, odd[None]]), kept, got, *extra)


def gather_tokens(array):
    n, k = lax.axis_size("row"), lax.axis_size("col")
    y = lax.axis_index("col")
    piece = array.shape[0] // k
    pieces = [lax.dynamic_slice_in_dim(array, (y ^ e) * piece, piece, axis=0) for e in range(k)]
    rows = [[p] for p in pieces]
    for d in range(1, n):
        own = swap(pieces[0], "row", d)
        rows[0].append(own)
        for e in range(1, k):
            rows[e].append(swap(own, "col", e))
    return jnp.concatenate([jnp.concatenate(r, axis=1) for r in rows], axis=0)


def join_dp(part, axis):
    for b in reversed(bits("dp")):
        part = jnp.concatenate([part, swap(part, "dp", b)], axis=axis)
    return part


def reduce_dp(part, axis):
    for b in bits("dp"):
        half = part.shape[axis] // 2
        keep = lax.slice_in_dim(part, 0, half, axis=axis)
        got = swap(lax.slice_in_dim(part, half, 2 * half, axis=axis), "dp", b)
        part = (keep.astype(F32) + got.astype(F32)).astype(BF16)
    return part


def spread(part, axis):
    n = lax.axis_size("row")
    block = part.shape[1 - axis] // n
    cut = [lax.slice_in_dim(part, d * block, (d + 1) * block, axis=1 - axis) for d in range(n)]
    mine = jnp.stack([cut[0]] + [swap(cut[d], "row", d) for d in range(1, n)])[None]
    order = list(reversed(bits("dp")))
    for b in order[:-1]:
        mine = jnp.concatenate([mine, swap(mine, "dp", b)], axis=0)
    return mine, swap(mine, "dp", order[-1])


def local(inputs, upstream, expand, biases, contract):
    n, k, q = lax.axis_size("row"), lax.axis_size("col"), lax.axis_size("dp")
    z, y, i = lax.axis_index("row"), lax.axis_index("col"), lax.axis_index("dp")
    tokens, block = inputs.shape
    width = expand.shape[1]
    factor = (tokens * q) ** (-0.5)
    own_width = width // n
    chunks = max(1, own_width // (q * LANES))
    chunk = own_width // chunks
    quarter = chunk // q
    order = dp_order()

    inputs_all = gather_tokens(inputs)
    upstream_all = gather_tokens(upstream)

    def source(c):
        far = [((z ^ d) * chunks + c) * q + i for d in range(1, n)]
        near = [(z * chunks + c) * q + (i ^ j) for j in order]
        return jnp.stack(far + near).astype(jnp.int32)

    def goal(c):
        half = order[: q // 2]
        return jnp.stack(
            [(((z ^ d) * chunks + c) * q + (i ^ j)) // 2 for d in range(n) for j in half]
        ).astype(jnp.int32)

    bias_rows = []
    grad_expand = grad_contract = share = None
    for c in range(chunks):
        index = source(c)
        *far_e, near_e = pick(expand, index, 1, quarter, n - 1)
        *far_c, near_c = pick(contract, index, 0, quarter, n - 1)
        rest_e = jnp.concatenate([swap(far_e[d - 1], "row", d) for d in range(1, n)], axis=0)
        rest_c = jnp.concatenate([swap(far_c[d - 1], "row", d) for d in range(1, n)], axis=1)
        expand_c = jnp.concatenate([near_e, join_dp(rest_e, 1)], axis=0)
        contract_c = jnp.concatenate([near_c, join_dp(rest_c, 0)], axis=1)
        near = [lax.dynamic_slice_in_dim(biases, index[n - 1 + t] * quarter, quarter) for t in range(q)]
        pre = dot(inputs_all, expand_c, 1, 0)
        back = dot(upstream_all, contract_c, 1, 1).astype(BF16)
        hidden = (pre + jnp.concatenate(near)[None, :]).astype(BF16)
        active, grad = pointwise(hidden, back)
        contract_part = (dot(active, upstream_all, 0, 0) * factor).astype(BF16)
        expand_part = (dot(inputs_all, grad, 0, 0) * factor).astype(BF16)
        bias_rows.append((jnp.sum(grad, axis=0, dtype=F32) * factor).astype(BF16).astype(F32))
        kept, got = spread(reduce_dp(contract_part, 0), 0)
        grad_contract = place(grad_contract, kept, got, goal(c), 0, contract.shape)
        kept, got = spread(reduce_dp(expand_part, 1), 1)
        grad_expand = place(grad_expand, kept, got, goal(c), 1, expand.shape)
        term = dot(grad, expand_c, 1, 1)
        share = term if share is None else share + term

    piece = tokens // k
    share = share.astype(BF16)
    total = share[:piece].astype(F32)
    for e in range(1, k):
        total = total + swap(share[e * piece : (e + 1) * piece], "col", e).astype(F32)
    total = total.astype(BF16)
    mine = total[:, :block].astype(F32)
    for d in range(1, n):
        mine = mine + swap(total[:, d * block : (d + 1) * block], "row", d).astype(F32)
    mine = mine.astype(BF16)
    grad_inputs = jnp.zeros((tokens, block), BF16)
    for e in range(k):
        got = mine if e == 0 else swap(mine, "col", e)
        grad_inputs = lax.dynamic_update_slice_in_dim(grad_inputs, got, (y ^ e) * piece, axis=0)

    vector = jnp.zeros((width + n * block,), F32)
    for c in range(chunks):
        for t, j in enumerate(order):
            at = (((z * chunks + c) * q) + (i ^ j)) * quarter
            vector = lax.dynamic_update_slice_in_dim(
                vector, bias_rows[c][t * quarter : (t + 1) * quarter], at, axis=0
            )
    offset = (jnp.sum(upstream, axis=0, dtype=F32) * factor).astype(BF16).astype(F32)
    vector = lax.dynamic_update_slice_in_dim(vector, offset, width + z * block, axis=0)
    vector = lax.psum(vector, ("row", "dp"))
    grad_biases = vector[:width].astype(BF16)
    grad_offset = lax.dynamic_slice_in_dim(vector, width + z * block, block, axis=0).astype(BF16)
    return (grad_inputs, grad_expand, grad_biases, grad_contract, grad_offset)


def fused_local(inputs, upstream, expand, biases, contract):
    n, k, q = lax.axis_size("row"), lax.axis_size("col"), lax.axis_size("dp")
    tokens, block = inputs.shape
    model = n * block
    width = expand.shape[1]
    own_width = width // n
    quarter = LANES
    chunk = q * quarter
    chunks = own_width // chunk
    half = tokens // k
    slots = 4
    parts = 2
    factor = (tokens * q) ** (-0.5)
    c0 = 0.7978845608028654
    c1 = 0.044715
    token_tile = 256 if tokens % 256 == 0 else tokens
    model_tile = 512 if block % 512 == 0 else block

    def kernel(
        x_ref, u_ref, e_ref, bias_ref, t_ref,
        gx_ref, ge_ref, gt_ref, gb_ref, go_ref,
        we_ref, wt_ref, r1e_ref, r1t_ref, r2e_ref, r2t_ref, s1_ref, s2_ref,
        x_all, u_all, e_buf, t_buf, act_t, hg, pe, pt, vecs, vecs_in, bias_all,
        line_s, line_r, y_s, y_r, send, recv, gy_s, gy_r, gi_s, gi_r, vec_s, vec_r, loc,
    ):
        z, y, i = lax.axis_index("row"), lax.axis_index("col"), lax.axis_index("dp")
        core, far = lax.rem(i, 2), lax.div(i, 2)
        r = core * 2 + far
        core_to = {"dp": far * 2 + (1 - core)}
        far_to = {"dp": (1 - far) * 2 + core}
        y_to = {"col": 1 - y}

        def row(d):
            return lax.rem(z + d, n)

        def span(start, size):
            return pl.ds(pl.multiple_of(start, size), size)

        def push(src, dst, ss, rs, to):
            pltpu.make_async_remote_copy(
                src_ref=src, dst_ref=dst, send_sem=ss, recv_sem=rs,
                device_id=to, device_id_type=pl.DeviceIdType.MESH,
            ).start()

        def wait(region, sem):
            pltpu.make_async_copy(region, region, sem).wait()

        barrier = pltpu.get_barrier_semaphore()
        partners = [{"row": row(d)} for d in range(1, n)] + [y_to, core_to, far_to]
        for to in partners:
            pl.semaphore_signal(barrier, inc=1, device_id=to, device_id_type=pl.DeviceIdType.MESH)
        pl.semaphore_wait(barrier, len(partners))

        arrays = ((x_ref, x_all), (u_ref, u_all))
        mine = span(y * half, half)
        own_loads = [
            pltpu.make_async_copy(a, full.at[:, span(z * block, block)], loc.at[m])
            for m, (a, full) in enumerate(arrays)
        ]
        for copy in own_loads:
            copy.start()

        wz, wx, wc, wf, rc, rx, az, ax, ac, af = range(10)

        def direct(c):
            return c >= 1 and c == chunks - 1

        def wide(c):
            return 2 * quarter if direct(c) else quarter

        def first(c):
            return core * 2 if direct(c) else r

        def weight_at(m, c, b, s):
            at = pl.ds(pl.multiple_of(s * quarter, quarter), wide(c))
            if m == 0:
                return we_ref.at[c, span(b * block, block), at]
            return wt_ref.at[c, at, span(b * block, block)]

        def weight_from(m, b, c):
            at = ((b * chunks + c) * q + first(c)) * quarter
            at = pl.ds(pl.multiple_of(at, quarter), wide(c))
            return e_ref.at[:, at] if m == 0 else t_ref.at[at, :]

        def weight_bytes(m, c):
            if m == 0:
                return we_ref.at[c, pl.ds(0, (n - 1) * block), pl.ds(0, wide(c))]
            return wt_ref.at[c, pl.ds(0, wide(c)), pl.ds(0, (n - 1) * block)]

        def send_weights(c, m):
            for d in range(1, n):
                push(weight_from(m, row(d), c), weight_at(m, c, z, first(c)),
                     send.at[wz, m, c], recv.at[wz, m, c], {"row": row(d)})

        def pass_weights(c, m):
            wait(weight_bytes(m, c), recv.at[wz, m, c])
            for stage, to in ((wx, far_to), (wc, core_to)):
                if stage == wx and direct(c):
                    continue
                for d in range(1, n):
                    at = weight_at(m, c, row(d), first(c))
                    push(at, at, send.at[stage, m, c], recv.at[stage, m, c], to)

        def hand_weights(c, m):
            if direct(c):
                return
            wait(weight_bytes(m, c), recv.at[wx, m, c])
            for d in range(1, n):
                at = weight_at(m, c, row(d), core * 2 + (1 - far))
                push(at, at, send.at[wf, m, c], recv.at[wf, m, c], core_to)

        part = half // parts

        def block_at(full, b, h):
            return full.at[span(y * half + h * part, part), span(b * block, block)]

        def other_at(full, b, h):
            return full.at[span((1 - y) * half + h * part, part), span(b * block, block)]

        ways = (
            (lambda s: z - s, lambda s: jnp.logical_and(z + 1 < n, z - s >= 0), 1,
             lambda s: z - 1 - s, lambda s: z - 1 - s >= 0),
            (lambda s: z + s, lambda s: jnp.logical_and(z >= 1, z + s < n), n - 1,
             lambda s: z + 1 + s, lambda s: z + 1 + s < n),
        )
        def line_send(m, s, h, w, src):
            sent, _, to, _, _ = ways[w]
            at = block_at(arrays[m][1], sent(s), h)
            push(at if src is None else src, at, line_s.at[m, w, s, h], line_r.at[m, w, s, h],
                 {"row": row(to)})

        def line_start(m):
            for h in range(parts):
                for w in range(2):

                    @pl.when(ways[w][1](0))
                    def _():
                        rows_at = span(y * half + h * part, part)
                        line_send(m, 0, h, w, arrays[m][0].at[rows_at, :])

        def line_take(m, s):
            for h in range(parts):
                for w, (_, sends, _, taken, takes) in enumerate(ways):

                    @pl.when(takes(s))
                    def _():
                        at = block_at(arrays[m][1], taken(s), h)
                        wait(at, line_r.at[m, w, s, h])
                        if s < n - 2:

                            @pl.when(sends(s + 1))
                            def _():
                                line_send(m, s + 1, h, w, None)

                        push(at, at, y_s.at[m, w, s, h], y_r.at[m, w, s, h], y_to)

        def line_join(m):
            for s in range(n - 1):
                for w, (_, _, _, taken, takes) in enumerate(ways):

                    @pl.when(takes(s))
                    def _():
                        for h in range(parts):
                            wait(other_at(arrays[m][1], taken(s), h), y_r.at[m, w, s, h])

        def line_end(m):
            full = arrays[m][1]
            for s in range(n - 1):
                for w, (sent, sends, _, taken, takes) in enumerate(ways):

                    @pl.when(sends(s))
                    def _():
                        for h in range(parts):
                            wait(block_at(full, sent(s), h), line_s.at[m, w, s, h])

                    @pl.when(takes(s))
                    def _():
                        for h in range(parts):
                            wait(block_at(full, taken(s), h), y_s.at[m, w, s, h])

        def load_weights(c, m):
            wait(weight_bytes(m, c), recv.at[wc, m, c])
            if not direct(c):
                wait(weight_bytes(m, c), recv.at[wf, m, c])
            copies = []
            for d in range(n):
                b = span(row(d) * block, block)
                at = span((row(d) * chunks + c) * chunk, chunk)
                if m == 0:
                    src = e_ref.at[:, at] if d == 0 else we_ref.at[c, b, :]
                    dst = e_buf.at[b, :]
                else:
                    src = t_ref.at[at, :] if d == 0 else wt_ref.at[c, :, b]
                    dst = t_buf.at[:, b]
                copies.append(pltpu.make_async_copy(src, dst, loc.at[d]))
            for copy in copies:
                copy.start()
            for copy in copies:
                copy.wait()

        def tanh_of(v, v2):
            return jnp.tanh(c0 * (v + c1 * (v2 * v)))

        def forward(c):
            load_weights(c, 0)
            bias = bias_ref[:, c * chunk : (c + 1) * chunk]

            def step(t, carry):
                at = span(t * token_tile, token_tile)
                pre = jnp.dot(x_all[at, :], e_buf[...], preferred_element_type=F32)
                hidden = (pre + bias).astype(BF16)
                hg[c, at, :] = hidden
                v = hidden.astype(F32)
                active = (0.5 * v * (1.0 + tanh_of(v, v * v))).astype(BF16)
                act_t[:, at] = active.T
                return carry

            lax.fori_loop(0, tokens // token_tile, step, 0)

        def backward(c):
            load_weights(c, 1)

            def step(t, total):
                at = span(t * token_tile, token_tile)
                back = dot(u_all[at, :], t_buf[...], 1, 1).astype(BF16).astype(F32)
                v = hg[c, at, :].astype(F32)
                v2 = v * v
                th = tanh_of(v, v2)
                slope = 0.5 * (1.0 + th) + 0.5 * v * (1.0 - th * th) * (c0 * (1.0 + (3.0 * c1) * v2))
                g = (back * slope).astype(BF16)
                hg[c, at, :] = g
                return total + jnp.sum(g.astype(F32), axis=0, keepdims=True)

            total = lax.fori_loop(0, tokens // token_tile, step, jnp.zeros((1, chunk), F32))
            vecs[0, :, c * chunk : (c + 1) * chunk] = (total * factor).astype(BF16).astype(F32)

        def offset():
            def step(t, total):
                at = span(t * token_tile, token_tile)
                part = u_all[at, span(z * block, block)].astype(F32)
                return total + jnp.sum(part, axis=0, keepdims=True)

            total = lax.fori_loop(0, tokens // token_tile, step, jnp.zeros((1, block), F32))
            vecs[0, :, own_width:] = (total * factor).astype(BF16).astype(F32)

        def bias_core():
            push(vecs.at[0], vecs_in.at[0], vec_s.at[0], vec_r.at[0], core_to)

        def bias_far():
            wait(vecs_in.at[0], vec_r.at[0])
            vecs[1] = vecs[0] + vecs_in[0]
            push(vecs.at[1], vecs_in.at[1], vec_s.at[1], vec_r.at[1], far_to)

        def bias_row():
            wait(vecs_in.at[1], vec_r.at[1])
            vecs[2] = vecs[1] + vecs_in[1]
            for d in range(1, n):
                push(vecs.at[2, :, pl.ds(0, own_width)], bias_all.at[z],
                     vec_s.at[2], vec_r.at[2], {"row": row(d)})
            bias_all[z] = vecs[2, :, :own_width]

        def bias_end():
            wait(bias_all.at[pl.ds(0, n - 1)], vec_r.at[2])
            gb_ref[...] = bias_all[...].astype(BF16)
            go_ref[...] = vecs[2, :, own_width:].astype(BF16)
            wait(bias_all.at[pl.ds(0, n - 1)], vec_s.at[2])
            wait(vecs.at[0], vec_s.at[0])
            wait(vecs.at[1], vec_s.at[1])

        def free_slot(c):
            slot = c % slots
            for m, part in enumerate((pe, pt)):
                wait(part.at[slot, pl.ds(0, 2)], send.at[rc, m, c])
                wait(part.at[slot, 0], send.at[rx, m, c])
                wait(zbytes(m, part, slot), send.at[az, m, c])

        def zbytes(m, part, slot):
            if m == 0:
                return part.at[slot, 0, pl.ds(0, (n - 1) * block), :]
            return part.at[slot, 0, :, pl.ds(0, (n - 1) * block)]

        other = pl.ds((1 - core) * 2, 2)

        def grads_t(c):
            slot = c % slots

            def step(t, carry):
                at = span(t * model_tile, model_tile)
                g = (jnp.dot(act_t[...], u_all[:, at], preferred_element_type=F32) * factor).astype(BF16)
                for j in range(q):
                    pt[slot, j, :, at] = g[j * quarter : (j + 1) * quarter, :]
                return carry

            lax.fori_loop(0, model // model_tile, step, 0)
            push(pt.at[slot, other], r1t_ref.at[c], send.at[rc, 1, c], recv.at[rc, 1, c], core_to)

        def grads_e(c):
            slot = c % slots

            def step(t, carry):
                at = span(t * model_tile, model_tile)
                g = (dot(x_all[:, at], hg[c], 0, 0) * factor).astype(BF16)
                for j in range(q):
                    pe[slot, j, at, :] = g[:, j * quarter : (j + 1) * quarter]
                return carry

            lax.fori_loop(0, model // model_tile, step, 0)
            push(pe.at[slot, other], r1e_ref.at[c], send.at[rc, 0, c], recv.at[rc, 0, c], core_to)

        def add_into(part, slot, j, got, tiles):
            rows = got.shape[0] // tiles

            def step(t, carry):
                at = span(t * rows, rows)
                total = part[slot, j, at, :].astype(F32) + got[at, :].astype(F32)
                part[slot, j, at, :] = total.astype(BF16)
                return carry

            lax.fori_loop(0, tiles, step, 0)

        sets = (
            (0, pe, [e_buf.at[:, pl.ds(h * quarter, quarter)] for h in range(2)], r1e_ref, r2e_ref),
            (1, pt, [t_buf.at[pl.ds(h * quarter, quarter), :] for h in range(2)], r1t_ref, r2t_ref),
        )

        def fetch(pairs):
            copies = [
                pltpu.make_async_copy(src, dst, loc.at[t]) for t, (src, dst) in enumerate(pairs)
            ]
            for copy in copies:
                copy.start()
            for copy in copies:
                copy.wait()


        def fold_core(c, which):
            slot = c % slots
            m, part, tmp, r1, r2 = sets[which]
            wait(r1.at[c], recv.at[rc, m, c])
            theirs = core * 2 + (1 - far)
            fetch([(r1.at[c, 1 - far], tmp[0]), (r1.at[c, far], tmp[1])])
            add_into(part, slot, theirs, tmp[0], 8)
            push(part.at[slot, theirs], r2.at[c], send.at[rx, m, c], recv.at[rx, m, c], far_to)
            add_into(part, slot, r, tmp[1], 8)

        def out_at(m, b, c, s):
            at = span(((b * chunks + c) * q + s) * quarter, quarter)
            return ge_ref.at[:, at] if m == 0 else gt_ref.at[at, :]

        def out_bytes(m, count):
            if m == 0:
                return ge_ref.at[:, pl.ds(0, count * quarter)]
            return gt_ref.at[pl.ds(0, count * quarter), :]

        def piece(m, part, slot, b):
            at = span(b * block, block)
            return part.at[slot, r, at, :] if m == 0 else part.at[slot, r, :, at]

        def fold_far(c, which):
            slot = c % slots
            m, part, tmp, r1, r2 = sets[which]
            wait(r2.at[c], recv.at[rx, m, c])
            fetch([(r2.at[c], tmp[0])])
            add_into(part, slot, r, tmp[0], 8)
            for d in range(1, n):
                push(piece(m, part, slot, row(d)), out_at(m, z, c, r),
                     send.at[az, m, c], recv.at[az, m, c], {"row": row(d)})
            copy = pltpu.make_async_copy(piece(m, part, slot, z), out_at(m, z, c, r), loc.at[0])
            copy.start()
            copy.wait()

        def pass_grads(c):
            for m in (1, 0):
                wait(out_bytes(m, n - 1), recv.at[az, m, c])
                for stage, to in ((ax, far_to), (ac, core_to)):
                    for d in range(n):
                        at = out_at(m, row(d), c, r)
                        push(at, at, send.at[stage, m, c], recv.at[stage, m, c], to)

        def hand_grads(c):
            for m in (1, 0):
                wait(out_bytes(m, n), recv.at[ax, m, c])
                for d in range(n):
                    at = out_at(m, row(d), c, core * 2 + (1 - far))
                    push(at, at, send.at[af, m, c], recv.at[af, m, c], core_to)

        theirs = span((1 - y) * half, half)

        def share_inputs(d):
            b = row(d)
            for piece_at in range(block // model_tile):
                start = pl.multiple_of(b * block + piece_at * model_tile, model_tile)
                copies = []
                for c in range(chunks):
                    if d == 0:
                        src = e_ref.at[pl.ds(piece_at * model_tile, model_tile),
                                       span((z * chunks + c) * chunk, chunk)]
                    else:
                        src = we_ref.at[c, pl.ds(start, model_tile), :]
                    copies.append(pltpu.make_async_copy(
                        src, e_buf.at[pl.ds(c * model_tile, model_tile), :], loc.at[c]))
                for copy in copies:
                    copy.start()
                for copy in copies:
                    copy.wait()

                def step(t, carry):
                    at = span(t * token_tile, token_tile)
                    total = jnp.zeros((token_tile, model_tile), F32)
                    for c in range(chunks):
                        w = e_buf[c * model_tile : (c + 1) * model_tile, :]
                        total = total + dot(hg[c, at, :], w, 1, 1)
                    x_all[at, pl.ds(start, model_tile)] = total.astype(BF16)
                    return carry

                lax.fori_loop(0, tokens // token_tile, step, 0)
            push(x_all.at[theirs, span(b * block, block)], s1_ref.at[d], gy_s.at[d], gy_r.at[d], y_to)

        rows = half // 8

        def fold_col(d):
            wait(s1_ref.at[d], gy_r.at[d])
            at_b = span(row(d) * block, block)
            got = t_buf.at[pl.ds(0, half), pl.ds(d * block, block)]
            copy = pltpu.make_async_copy(s1_ref.at[d], got, loc.at[0])
            copy.start()
            copy.wait()

            def step(t, carry):
                at = pl.ds(pl.multiple_of(y * half + t * rows, rows), rows)
                here = span(t * rows, rows)
                total = x_all[at, at_b].astype(F32) + got[here, :].astype(F32)
                x_all[at, at_b] = total.astype(BF16)
                return carry

            lax.fori_loop(0, 8, step, 0)
            if d > 0:
                push(x_all.at[mine, at_b], s2_ref.at[d - 1], gi_s.at[0], gi_r.at[0], {"row": row(d)})

        def fold_row():
            wait(s2_ref, gi_r.at[0])
            copies = []
            for d in range(1, n):
                copies.append(pltpu.make_async_copy(
                    s2_ref.at[d - 1], t_buf.at[pl.ds(0, half), pl.ds((d - 1) * block, block)],
                    loc.at[d]))
            for copy in copies:
                copy.start()
            for copy in copies:
                copy.wait()
            at_z = span(z * block, block)

            def step(t, carry):
                at = pl.ds(pl.multiple_of(y * half + t * rows, rows), rows)
                here = span(t * rows, rows)
                total = x_all[at, at_z].astype(F32)
                for d in range(1, n):
                    total = total + t_buf[here, pl.ds((d - 1) * block, block)].astype(F32)
                x_all[at, at_z] = total.astype(BF16)
                return carry

            lax.fori_loop(0, 8, step, 0)
            src = x_all.at[mine, at_z]
            push(src, gx_ref.at[mine, :], gi_s.at[1], gi_r.at[1], y_to)
            copy = pltpu.make_async_copy(src, gx_ref.at[mine, :], loc.at[0])
            copy.start()
            copy.wait()

        last = chunks - 1
        edge = n - 2

        line_start(0)
        send_weights(0, 0)
        for s in range(n - 1):
            if s == edge:
                line_start(1)
            line_take(0, s)
            if s == 0:
                pass_weights(0, 0)
        hand_weights(0, 0)
        for copy in own_loads:
            copy.wait()
        at_end = jnp.logical_or(z == 0, z == n - 1)
        for s in range(n - 1):
            if s == min(1, edge):
                line_join(0)
                forward(0)
                offset()
            line_take(1, s)
            if s == 0:

                @pl.when(at_end)
                def _():
                    send_weights(0, 1)

        line_join(1)

        for c in range(chunks):
            if c > 0:
                forward(c)
            if c >= slots:
                free_slot(c - slots)
            grads_t(c)
            if c == 0:

                @pl.when(jnp.logical_not(at_end))
                def _():
                    send_weights(0, 1)

                for m in range(2):
                    if chunks > 1:
                        send_weights(1, m)
                pass_weights(0, 1)
                fold_core(0, 1)
                for later in range(2, chunks):
                    for m in range(2):
                        send_weights(later, m)
                hand_weights(0, 1)
            backward(c)
            if c > 0:
                fold_core(c, 1)
            if c + 1 < chunks and c >= 2:
                pass_weights(c + 1, 1)
            if c >= 3:
                pass_grads(c - 3)
            grads_e(c)
            if c == 0 and chunks > 1:
                pass_weights(1, 0)
                pass_weights(1, 1)
            if c == last:
                bias_core()
            fold_core(c, 0)
            if c + 1 < chunks:
                hand_weights(c + 1, 0)
                hand_weights(c + 1, 1)
            if c + 2 < chunks:
                pass_weights(c + 2, 0)
                if c == 0:
                    pass_weights(c + 2, 1)
            if c >= 1:
                fold_far(c - 1, 1)
                fold_far(c - 1, 0)
        done = max(0, last - 2)
        handed = 0
        bias_far()
        line_end(0)
        for d in range(1, n):
            if d == 1 and done < last - 1:
                pass_grads(done)
                done += 1
            share_inputs(d)
        share_inputs(0)
        fold_col(1)
        if done < last:
            pass_grads(done)
            done += 1
        fold_far(last, 1)
        fold_far(last, 0)
        for d in list(range(2, n)) + [0]:
            fold_col(d)
        for c in range(last - 1):
            hand_grads(c)
        while done <= last:
            pass_grads(done)
            done += 1
        fold_row()
        bias_row()
        for c in range(max(0, last - 1), chunks):
            hand_grads(c)
        bias_end()

        for c in range(max(0, chunks - slots), chunks):
            free_slot(c)
        for c in range(chunks):
            for m in range(2):
                for stage in (wz, wc) if direct(c) else (wz, wx, wc, wf):
                    wait(weight_bytes(m, c), send.at[stage, m, c])
                for stage in (ax, ac, af):
                    wait(out_bytes(m, n), send.at[stage, m, c])
                for stage in (ac, af):
                    wait(out_bytes(m, n), recv.at[stage, m, c])
        for d in range(n):
            wait(s1_ref.at[d], gy_s.at[d])
        wait(s2_ref, gi_s.at[0])
        wait(gx_ref.at[mine, :], gi_s.at[1])
        wait(gx_ref.at[mine, :], gi_r.at[1])
        line_end(1)

    hbm = pl.BlockSpec(memory_space=pl.ANY)
    vmem = pl.BlockSpec(memory_space=pltpu.VMEM)
    z = lax.axis_index("row")
    own_bias = lax.dynamic_slice_in_dim(biases, z * own_width, own_width)[None]
    shaped = lambda *shape: jax.ShapeDtypeStruct(shape, BF16)
    dma = pltpu.SemaphoreType.DMA
    flops = 10 * tokens * model * own_width
    outs = pl.pallas_call(
        kernel,
        in_specs=[hbm, hbm, hbm, vmem, hbm],
        out_specs=[hbm, hbm, hbm, vmem, vmem] + [hbm] * 8,
        out_shape=[
            shaped(tokens, block),
            shaped(block, width),
            shaped(width, block),
            shaped(n, 1, own_width),
            shaped(1, block),
            shaped(chunks, model, chunk),
            shaped(chunks, chunk, model),
            shaped(chunks, 2, model, quarter),
            shaped(chunks, 2, quarter, model),
            shaped(chunks, model, quarter),
            shaped(chunks, quarter, model),
            shaped(n, half, block),
            shaped(n - 1, half, block),
        ],
        scratch_shapes=[
            pltpu.VMEM((tokens, model), BF16),
            pltpu.VMEM((tokens, model), BF16),
            pltpu.VMEM((model, chunk), BF16),
            pltpu.VMEM((chunk, model), BF16),
            pltpu.VMEM((chunk, tokens), BF16),
            pltpu.VMEM((chunks, tokens, chunk), BF16),
            pltpu.VMEM((slots, q, model, quarter), BF16),
            pltpu.VMEM((slots, q, quarter, model), BF16),
            pltpu.VMEM((3, 1, own_width + block), F32),
            pltpu.VMEM((2, 1, own_width + block), F32),
            pltpu.VMEM((n, 1, own_width), F32),
            dma((2, 2, n - 1, parts)),
            dma((2, 2, n - 1, parts)),
            dma((2, 2, n - 1, parts)),
            dma((2, 2, n - 1, parts)),
            dma((10, 2, chunks)),
            dma((10, 2, chunks)),
            dma((n,)),
            dma((n,)),
            dma((2,)),
            dma((2,)),
            dma((3,)),
            dma((3,)),
            dma((max(n, chunks),)),
        ],
        compiler_params=pltpu.CompilerParams(
            collective_id=0, has_side_effects=True, vmem_limit_bytes=67_000_000
        ),
        cost_estimate=pl.CostEstimate(flops=flops, bytes_accessed=200_000_000, transcendentals=0),
        name="fused",
    )(inputs, upstream, expand, own_bias, contract)
    grad_inputs, grad_expand, grad_contract, grad_biases, grad_offset = outs[:5]
    return (
        grad_inputs,
        grad_expand,
        grad_biases.reshape(width),
        grad_contract,
        grad_offset.reshape(block),
    )


def program(inputs, upstream, expand, biases, contract):
    n, k, q = lax.axis_size("row"), lax.axis_size("col"), lax.axis_size("dp")
    tokens, block = inputs.shape
    own_width = expand.shape[1] // n
    fits = q == 4 and k == 2 and n > 1 and own_width % (q * LANES) == 0
    fits = fits and tokens % 512 == 0 and block % 512 == 0 and tokens // k <= q * LANES
    body = fused_local if fits else local
    return body(inputs, upstream, expand, biases, contract)


def solution(mesh):
    in_specs = (P("dp", "row"), P("dp", "row"), P("row", "col"), P("col"), P("col", "row"))
    out_specs = (P("dp", "row"), P("row", "col"), P("col"), P("col", "row"), P("row"))
    return jax.shard_map(program, mesh=mesh, in_specs=in_specs, out_specs=out_specs, check_vma=False)
```
